32 devices in a mesh: grp: 4 (over y, x), dev: 8 (over z, core).
Axes of the slice: x: 2, y: 2, z: 4, core: 2. Of those that a mesh axis runs over, the one named last changes fastest.
Arguments:
- points: bfloat16 [65536, 256], P(('grp', 'dev')), may hold values from -6 to 6
- ridge: float32 [1024], replicated, may hold values from 0.25 to 2
- landmark_ids: int32 [1024], replicated, may hold values from 0 to 65535, as said below
Outputs:
- features: bfloat16 [65536, 1024], P(('grp', 'dev'))
The draws below stay inside these ranges and needn't reach their ends.
Inputs may be any that keep to these rules, and one draw needn't show every extreme that they name: `landmark_ids`: sorted ascending, all distinct.
All inputs are finite; a program needn't handle non-finite values.
Results may differ from the reference program's by a relative error of at most 0.0015.
Values may be sent and summed in bfloat16 or wider, within the bound.
No kernel may reach another device: no remote copies, remote signals or barrier semaphores. Data moves between devices by JAX's collectives and lax.ppermute only.
A program may use at most 128 MiB of HBM per device.

```python
import math
import jax
import jax.numpy as jnp
from jax import lax

D = 256
M = 1024
ROWS = 2048
NPTS = 65536


def draw_landmark_ids(key, part):
    order = jax.random.permutation(jax.random.fold_in(key, 11), NPTS)
    return jnp.sort(order[:M]).astype(jnp.int32)


def block_levels(rng, dims, split, low, largest):
    level = 1.0
    for dim, parts in split:
        steps = jax.random.uniform(jax.random.fold_in(jax.random.fold_in(rng, 6), dim), (parts,), jnp.float32, low / len(split), largest / len(split))
        level = level * jnp.repeat(jnp.exp(steps), dims[dim] // parts).reshape((-1,) + (1,) * (len(dims) - 1 - dim))
    return level


def gaussian(rng, shape, deviation, limit, shards=(), dtype=jnp.bfloat16):
    values = deviation * jax.random.normal(rng, shape, jnp.float32)
    if shards:
        values = values * block_levels(rng, shape, shards, -0.22, 0.18)
    return jnp.clip(values, -limit, limit).astype(dtype)


def setup_inputs(seed: int = 0) -> dict:
    seeds = jax.random.split(jax.random.key(seed), 4)
    return {
        "points": gaussian(seeds[0], (NPTS, D), 1.0, 6.0, ((0, 32),)),
        "ridge": jnp.clip(jnp.exp(jax.random.uniform(seeds[1], (M,), jnp.float32, math.log(0.25), math.log(2.0))), 0.25, 2.0),
        "landmark_ids": draw_landmark_ids(jax.random.fold_in(seeds[3], 71), 0),
    }


def kernel_block(left, right):
    left_sq = lax.optimization_barrier(jnp.sum(jnp.square(left.astype(jnp.float32)), axis=1))
    right_sq = lax.optimization_barrier(jnp.sum(jnp.square(right.astype(jnp.float32)), axis=1))
    inner = jnp.dot(left.astype(jnp.float32), right.T.astype(jnp.float32), preferred_element_type=jnp.float32)
    return jnp.exp(-(left_sq[:, None] + right_sq[None, :] - 2.0 * inner) / (2.0 * D))

def reference(points, ridge, landmark_ids):
    marks = points[landmark_ids.astype(jnp.int32)]
    core = kernel_block(marks, marks) + jnp.diag(ridge)
    lower = jnp.linalg.cholesky(core)

    def one_block(block):
        cross = kernel_block(block, marks)
        return lax.linalg.triangular_solve(lower, cross, left_side=False, lower=True, transpose_a=True)
    blocks = points.reshape(NPTS // ROWS, ROWS, D)
    raw = lax.map(one_block, blocks).reshape(NPTS, M)
    mean = lax.optimization_barrier(jnp.mean(raw, axis=0))
    var = lax.optimization_barrier(jnp.mean(jnp.square(raw - mean[None, :]), axis=0))
    return ((raw - mean[None, :]) / jnp.sqrt(var + 1e-05)[None, :]).astype(jnp.bfloat16)
```

```python
import functools
import math

import jax
import jax.numpy as jnp
from jax import lax
from jax.experimental import pallas as pl
from jax.experimental.pallas import tpu as pltpu
from jax.sharding import PartitionSpec as P

AXES = ("grp", "dev")
B = 128
S = 256
TILE = 512


def split(x):
    hi = x.astype(jnp.bfloat16)
    return hi, (x - hi.astype(jnp.float32)).astype(jnp.bfloat16)


def dot_nt(left, right):
    return lax.dot_general(left, right, (((1,), (1,)), ((), ())), preferred_element_type=jnp.float32)


def left3(x):
    hi, lo = split(x)
    return jnp.concatenate([hi, lo, hi], axis=1)


def right3(x):
    hi, lo = split(x)
    return jnp.concatenate([hi, hi, lo], axis=1)


def factor_block(a_ref, sub, lane):
    n = B // 8
    rows = [a_ref[8 * t:8 * t + 8, :] for t in range(n)]
    out = []
    for k in range(n):
        first = 8 * k
        group = rows[k]
        cols = [jnp.broadcast_to(group[:, first + b:first + b + 1], (8, B)) for b in range(8)]
        below = {
            t: [jnp.broadcast_to(rows[t][:, first + j:first + j + 1], (8, B)) for j in range(8)]
            for t in range(k + 1, n)
        }
        pivot = (lane >= first) & (lane < first + 8)
        start = jnp.where(pivot, (lane - first == sub).astype(jnp.float32), group)
        s = {(a, b): jnp.broadcast_to(cols[b][a:a + 1, :], (8, B)) for b in range(8) for a in range(b + 1)}
        y = [jnp.broadcast_to(start[i:i + 1, :], (8, B)) for i in range(8)]
        follow = k + 1 < n
        if follow:
            z = list(below[k + 1])
            acc = jnp.where(pivot, 0.0, rows[k + 1])
        inv = []
        for j in range(8):
            r = lax.rsqrt(s[(j, j)])
            inv.append(r)
            for b in range(j + 1, 8):
                s[(j, b)] = s[(j, b)] * r
            y[j] = y[j] * r
            if follow:
                z[j] = z[j] * r
                acc = acc - z[j] * y[j]
            for b in range(j + 1, 8):
                for a in range(j + 1, b + 1):
                    s[(a, b)] = s[(a, b)] - s[(j, a)] * s[(j, b)]
            for b in range(j + 1, 8):
                y[b] = y[b] - s[(j, b)] * y[j]
                if follow:
                    z[b] = z[b] - s[(j, b)] * z[j]
        w = y[7]
        for i in range(7):
            w = jnp.where(sub == i, y[i], w)
        out.append(jnp.where(lane < first + 8, w, 0.0))
        if follow:
            rows[k + 1] = acc
        if k + 2 < n:
            q = [None] * 8
            for j in range(7, -1, -1):
                v = y[j]
                for i in range(j + 1, 8):
                    v = v - s[(j, i)] * q[i]
                q[j] = v * inv[j]
            for t in range(k + 2, n):
                v = jnp.where(pivot, 0.0, rows[t])
                for j in range(8):
                    v = v - below[t][j] * q[j]
                rows[t] = v
    return out


def square_sums(x):
    hi, lo = split(jnp.square(x.astype(jnp.float32)))
    both = jnp.concatenate([hi, lo], axis=1)
    return dot_nt(jnp.ones((8, both.shape[1]), jnp.bfloat16), both), dot_nt(both, jnp.ones((B, both.shape[1]), jnp.bfloat16))


def factor(a_ref, d_ref, w3_ref, l3_ref):
    nb, m, _ = a_ref.shape
    sub = lax.broadcasted_iota(jnp.int32, (8, B), 0)
    lane = lax.broadcasted_iota(jnp.int32, (8, B), 1)

    def panel(p, carry):
        d_ref[0] = a_ref[p, pl.ds(pl.multiple_of(p * B, B), B), :]
        for k, rows in enumerate(factor_block(d_ref.at[0], sub, lane)):
            d_ref[0, 8 * k:8 * k + 8, :] = rows

        def finish(q):
            w = d_ref[0]
            top = (q + 1) * B
            step, odd = divmod(q, S // B)
            if top < m:
                block = dot_nt(left3(a_ref[q, top:, :]), right3(w))
                hi, lo = split(block)
                if (step + 1) * S < m:
                    at = step * 3 * S + odd * B
                    l3_ref[top:, at:at + B] = hi
                    l3_ref[top:, at + S:at + S + B] = hi
                    l3_ref[top:, at + 2 * S:at + 2 * S + B] = lo
                left = jnp.concatenate([hi, lo, hi], axis=1)
                right = jnp.concatenate([hi, hi, lo], axis=1)
                for j in range(q + 1, nb):
                    o = (j - q - 1) * B
                    a_ref[j, j * B:, :] -= dot_nt(left[o:], right[o:o + B])
            if odd == 0:
                d_ref[1] = w
                d_ref[2] = block[:B]
            else:
                w0 = d_ref[1]
                inner = lax.dot_general(left3(d_ref[2]), jnp.concatenate([split(w0)[0], split(w0)[0], split(w0)[1]], axis=0), (((1,), (0,)), ((), ())), preferred_element_type=jnp.float32)
                hi, lo = split(inner)
                corner = -lax.dot_general(left3(w), jnp.concatenate([hi, hi, lo], axis=0), (((1,), (0,)), ((), ())), preferred_element_type=jnp.float32)
                upper = jnp.concatenate([w0, jnp.zeros_like(w0)], axis=1)
                lower = jnp.concatenate([corner, w], axis=1)
                w3_ref[step * S:(step + 1) * S, :] = right3(jnp.concatenate([upper, lower], axis=0))

        for q in range(nb):
            pl.when(p == q)(functools.partial(finish, q))
        return carry

    lax.fori_loop(0, nb, panel, 0)


def kernel(src_ref, dst_ref, rows_ref, points_ref, ridge_ref, raw_ref, stat_ref,
           marks_ref, packed_ref, a_ref, d_ref, w3_ref, l3_ref, r3_ref):
    i = pl.program_id(0)
    m, width = marks_ref.shape
    scale = 1.0 / (2.0 * width)
    cap = packed_ref.shape[1] - m

    @pl.when(i == 0)
    def _():
        def place(d, carry):
            rows = rows_ref[pl.ds(pl.multiple_of(src_ref[d] * cap, cap), cap), :].astype(jnp.float32)
            for c in range(width // B):
                packed_ref[c, pl.ds(dst_ref[d], cap), :] = rows[:, c * B:(c + 1) * B]
            return carry
        lax.fori_loop(0, src_ref.shape[0], place, 0)
        marks_ref[...] = jnp.concatenate([packed_ref[c, :m] for c in range(width // B)], axis=1).astype(jnp.bfloat16)
        marks = marks_ref[...]
        along, down = square_sums(marks)
        stat_ref[...] = jnp.zeros_like(stat_ref)
        d_ref[3, 0:8, :] = jnp.zeros((8, B), jnp.float32)
        for j in range(m // B):
            inner = dot_nt(marks, marks[j * B:(j + 1) * B])
            block = jnp.exp(-(down + along[0:1, j * B:(j + 1) * B] - 2.0 * inner) * scale)
            a_ref[j] = block
            row = lax.broadcasted_iota(jnp.int32, (B, B), 0)
            col = lax.broadcasted_iota(jnp.int32, (B, B), 1)
            a_ref[j, j * B:(j + 1) * B, :] += jnp.where(row == col, ridge_ref[0:1, j * B:(j + 1) * B], 0.0)
        factor(a_ref, d_ref, w3_ref, l3_ref)

    points = points_ref[...]
    _, down = square_sums(points)
    down = jnp.concatenate([down] * (S // B), axis=1)
    marks = marks_ref[...]
    along, _ = square_sums(marks)
    count = points.shape[0]
    before = (i * count).astype(jnp.float32)
    share = count / (before + count)
    for p in range(m // S):
        here = slice(p * S, (p + 1) * S)
        inner = dot_nt(points, marks[here])
        cross = jnp.exp(-(down + along[0:1, here] - 2.0 * inner) * scale)
        if p:
            cross = cross - dot_nt(r3_ref[:, :p * 3 * S], l3_ref[here, :p * 3 * S])
        raw = dot_nt(left3(cross), w3_ref[here, :])
        raw_ref[:, here] = raw
        if p + 1 < m // S:
            r3_ref[:, p * 3 * S:(p + 1) * 3 * S] = left3(raw)
        mean = jnp.mean(raw, axis=0, keepdims=True)
        spread = jnp.sum(jnp.square(raw - mean), axis=0, keepdims=True)
        delta = mean - stat_ref[0:1, here]
        stat_ref[1:2, here] += spread + jnp.square(delta) * (before * share)
        stat_ref[0:1, here] += delta * share


def exchange(x, bit):
    dev = lax.axis_size("dev")
    axis, flip = ("dev", bit) if bit < dev else ("grp", bit // dev)
    size = lax.axis_size(axis)
    return lax.ppermute(x, axis, [(k, k ^ flip) for k in range(size)])


def shards(points, ridge, landmark_ids):
    count, width = points.shape
    m = landmark_ids.shape[0]
    devices = lax.axis_size(AXES)
    me = lax.axis_index(AXES)
    mean = m / devices
    cap = min(m, 16 * math.ceil((mean + 5.6 * math.sqrt(mean)) / 16))
    bits = [1 << b for b in range(devices.bit_length() - 1)]
    order = bits[1:] + bits[:1]

    bounds = jnp.sum(landmark_ids[None, :] < (jnp.arange(devices + 1) * count)[:, None], axis=1, dtype=jnp.int32)
    low = bounds[:-1]
    fits = jnp.max(bounds[1:] - low) <= cap

    def packed(points, ids):
        mine = lax.dynamic_slice(jnp.pad(ids, (0, cap)), (low[me],), (cap,))
        rows = points[jnp.clip(mine - me * count, 0, count - 1)]
        for bit in order:
            rows = jnp.concatenate([rows, exchange(rows, bit)], axis=0)
        far = jnp.arange(devices, dtype=jnp.int32) ^ me
        place = jnp.zeros_like(far)
        for k, bit in enumerate(order):
            place = place + jnp.where((far & bit) != 0, 1 << k, 0)
        return rows, place, low

    def summed(points, ids):
        offset = ids - me * count
        inside = (offset >= 0) & (offset < count)
        picked = points[jnp.clip(offset, 0, count - 1)]
        rows = lax.psum(jnp.where(inside[:, None], picked.astype(jnp.float32), 0.0), AXES).astype(points.dtype)
        rows = jnp.pad(rows, ((0, max(0, devices * cap - m)), (0, 0)))
        place = jnp.arange(devices, dtype=jnp.int32) % (m // cap)
        return rows, place, place * cap

    rows, src, dst = lax.cond(fits, packed, summed, points, landmark_ids)

    raw, stat = pl.pallas_call(
        kernel,
        grid_spec=pltpu.PrefetchScalarGridSpec(
            num_scalar_prefetch=2,
            grid=(count // TILE,),
            in_specs=[
                pl.BlockSpec(rows.shape, lambda i, *_: (0, 0), pipeline_mode=pl.Buffered(1)),
                pl.BlockSpec((TILE, width), lambda i, *_: (i, 0)),
                pl.BlockSpec((1, m), lambda i, *_: (0, 0)),
            ],
            out_specs=[
                pl.BlockSpec((TILE, m), lambda i, *_: (i, 0)),
                pl.BlockSpec((8, m), lambda i, *_: (0, 0)),
            ],
            scratch_shapes=[
                pltpu.VMEM((m, width), jnp.bfloat16),
                pltpu.VMEM((width // B, m + cap, B), jnp.float32),
                pltpu.VMEM((m // B, m, B), jnp.float32),
                pltpu.VMEM((4, B, B), jnp.float32),
                pltpu.VMEM((m, 3 * S), jnp.bfloat16),
                pltpu.VMEM((m, 3 * (m - S)), jnp.bfloat16),
                pltpu.VMEM((TILE, 3 * (m - S)), jnp.bfloat16),
            ],
        ),
        out_shape=(jax.ShapeDtypeStruct((count, m), jnp.float32), jax.ShapeDtypeStruct((8, m), jnp.float32)),
        compiler_params=pltpu.CompilerParams(vmem_limit_bytes=60 << 20, dimension_semantics=("arbitrary",)),
        name="nystrom",
    )(src, dst, rows, points, ridge[None, :])

    stat = stat[:2]
    total = count
    for bit in bits:
        other = exchange(stat, bit)
        delta = other[0] - stat[0]
        stat = jnp.stack([0.5 * (stat[0] + other[0]), stat[1] + other[1] + jnp.square(delta) * (0.5 * total)])
        total *= 2
    var = stat[1] / total
    return ((raw - stat[0][None, :]) / jnp.sqrt(var + 1e-05)[None, :]).astype(jnp.bfloat16)


def solution(mesh):
    placed = (P(AXES, None), P(), P())
    return jax.shard_map(shards, mesh=mesh, in_specs=placed, out_specs=P(AXES, None), check_vma=False)
```

```python
import functools
import math

import jax
import jax.numpy as jnp
from jax import lax
from jax.experimental import pallas as pl
from jax.experimental.pallas import tpu as pltpu
from jax.sharding import PartitionSpec as P

AXES = ("grp", "dev")
B = 128
S = 256
ROWS = 512


def split(x):
    hi = x.astype(jnp.bfloat16)
    return hi, (x - hi.astype(jnp.float32)).astype(jnp.bfloat16)


def dot(left, right, dims=((1,), (0,))):
    return lax.dot_general(left, right, (dims, ((), ())), preferred_element_type=jnp.float32)


def dot_nt(left, right):
    return dot(left, right, ((1,), (1,)))


def dot3(left, right):
    return dot(left[0], right[0]) + dot(left[1], right[0]) + dot(left[0], right[1])


def dot3_narrow(left, right):
    left = jnp.concatenate([left[0], left[1], left[0]], axis=1)
    right = jnp.concatenate([right[0], right[0], right[1]], axis=0)
    return dot(left, right)


def factor_block(d_ref, c_ref, sub, lane):
    n = B // 8
    rows = [d_ref[8 * t:8 * t + 8, :] for t in range(n)]
    for k in range(n):
        first = 8 * k
        group = rows[k]
        slot = (k % 2) * 64
        for b in range(8):
            c_ref[slot + 8 * b:slot + 8 * b + 8, :] = jnp.broadcast_to(group[:, first + b:first + b + 1], (8, B))
        below = {
            t: [jnp.broadcast_to(rows[t][:, first + j:first + j + 1], (8, B)) for j in range(8)]
            for t in range(k + 1, n)
        }
        pivot = (lane >= first) & (lane < first + 8)
        start = jnp.where(pivot, (lane - first == sub).astype(jnp.float32), group)
        s = {}
        for b in range(8):
            for a in range(b + 1):
                at = slot + 8 * b + a
                s[(a, b)] = jnp.broadcast_to(c_ref[at:at + 1, :], (8, B))
        y = [jnp.broadcast_to(start[i:i + 1, :], (8, B)) for i in range(8)]
        follow = k + 1 < n
        if follow:
            z = list(below[k + 1])
            acc = jnp.where(pivot, 0.0, rows[k + 1])
        inv = []
        for j in range(8):
            r = lax.rsqrt(s[(j, j)])
            inv.append(r)
            for b in range(j + 1, 8):
                s[(j, b)] = s[(j, b)] * r
            y[j] = y[j] * r
            if follow:
                z[j] = z[j] * r
                acc = acc - z[j] * y[j]
            for b in range(j + 1, 8):
                for a in range(j + 1, b + 1):
                    s[(a, b)] = s[(a, b)] - s[(j, a)] * s[(j, b)]
            for b in range(j + 1, 8):
                y[b] = y[b] - s[(j, b)] * y[j]
                if follow:
                    z[b] = z[b] - s[(j, b)] * z[j]
        w = y[7]
        for i in range(7):
            w = jnp.where(sub == i, y[i], w)
        d_ref[first:first + 8, :] = jnp.where(lane < first + 8, w, 0.0)
        if follow:
            rows[k + 1] = acc
        if k + 2 < n:
            q = [None] * 8
            for j in range(7, -1, -1):
                v = y[j]
                for i in range(j + 1, 8):
                    v = v - s[(j, i)] * q[i]
                q[j] = v * inv[j]
            for t in range(k + 2, n):
                v = jnp.where(pivot, 0.0, rows[t])
                for j in range(8):
                    v = v - below[t][j] * q[j]
                rows[t] = v
        yield k


def square_sums(x):
    hi, lo = split(jnp.square(x.astype(jnp.float32)))
    both = jnp.concatenate([hi, lo], axis=1)
    return dot_nt(jnp.ones((8, both.shape[1]), jnp.bfloat16), both), dot_nt(both, jnp.ones((B, both.shape[1]), jnp.bfloat16))


def wide(x):
    return jnp.concatenate([x] * (S // B), axis=1)


def kernel(src_ref, dst_ref, rows_ref, points_ref, ridge_ref, raw_hbm, stat_ref,
           marks_ref, packed_ref, along_ref, a_ref, d_ref, c_ref, l_ref, lt_ref, wt_ref, x_ref, r_ref, sems):
    m, width = marks_ref.shape
    count = points_ref.shape[0]
    scale = 1.0 / (2.0 * width)
    cap = packed_ref.shape[1] - m
    stages = m // S
    half = count // 2
    sub = lax.broadcasted_iota(jnp.int32, (8, B), 0)
    lane = lax.broadcasted_iota(jnp.int32, (8, B), 1)

    def place(d, carry):
        rows = rows_ref[pl.ds(pl.multiple_of(src_ref[d] * cap, cap), cap), :].astype(jnp.float32)
        for c in range(width // B):
            packed_ref[c, pl.ds(dst_ref[d], cap), :] = rows[:, c * B:(c + 1) * B]
        return carry

    lax.fori_loop(0, src_ref.shape[0], place, 0)
    marks_ref[...] = jnp.concatenate([packed_ref[c, :m] for c in range(width // B)], axis=1).astype(jnp.bfloat16)
    marks = marks_ref[...]
    along, down = square_sums(marks)
    along_ref[...] = along
    down = wide(down)
    stat_ref[...] = jnp.zeros_like(stat_ref)
    row = lax.broadcasted_iota(jnp.int32, (S, S), 0)
    col = lax.broadcasted_iota(jnp.int32, (S, S), 1)
    for j in range(stages):
        here = slice(j * S, (j + 1) * S)
        inner = dot_nt(marks[j * S:], marks[here])
        a_ref[j, j * S:, :] = jnp.exp(-(down[j * S:] + along[0:1, here] - 2.0 * inner) * scale)
        a_ref[j, here, :] += jnp.where(row == col, ridge_ref[0:1, here], 0.0)
    d_ref[0] = a_ref[0, :B, :B]

    def copy(p, odd):
        rows = pl.ds(pl.multiple_of(odd * half, half), half)
        return pltpu.make_async_copy(x_ref.at[p, rows, :], raw_hbm.at[rows, pl.ds(p * S, S)], sems.at[p, odd])

    def cross_piece(j, at):
        here = slice(j * S, (j + 1) * S)
        rows = pl.ds(at, ROWS)
        points = points_ref[rows, :]
        _, down = square_sums(points)
        inner = dot_nt(points, marks_ref[here, :])
        x_ref[j, rows, :] = jnp.exp(-(wide(down) + along_ref[0:1, here] - 2.0 * inner) * scale)

    def raw_piece(p, at):
        here = slice(p * S, (p + 1) * S)
        rows = pl.ds(at, ROWS)
        raw = dot3(split(x_ref[p, rows, :]), (wt_ref[0], wt_ref[1]))
        x_ref[p, rows, :] = raw
        r_ref[0, rows, :], r_ref[1, rows, :] = split(raw)
        mean = jnp.mean(raw, axis=0, keepdims=True)
        spread = jnp.sum(jnp.square(raw - mean), axis=0, keepdims=True)
        before = jnp.asarray(at).astype(jnp.float32)
        share = ROWS / (before + ROWS)
        delta = mean - stat_ref[0:1, here]
        stat_ref[1:2, here] += spread + jnp.square(delta) * (before * share)
        stat_ref[0:1, here] += delta * share

    def update_piece(p, j, at):
        rows = pl.ds(at, ROWS)
        right = [lt_ref[h, p * S:(p + 1) * S, j * S:(j + 1) * S] for h in range(2)]
        x_ref[j, rows, :] -= dot3((r_ref[0, rows, :], r_ref[1, rows, :]), right)

    def core_piece(p, j, odd):
        size = (m - j * S) // 2
        rows = pl.ds(pl.multiple_of(j * S + odd * size, B), size)
        right = [lt_ref[h, p * S:(p + 1) * S, j * S:(j + 1) * S] for h in range(2)]
        keep = 2 * (p % 2)
        a_ref[j, rows, :] -= dot3((l_ref[keep, rows, :], l_ref[keep + 1, rows, :]), right)

    def finish(p, odd):
        top = p * S + (odd + 1) * B
        here = slice(odd * B, (odd + 1) * B)
        at = slice(p * S + odd * B, p * S + (odd + 1) * B)
        keep = 2 * (p % 2)
        wt = jnp.transpose(d_ref[0])
        if top < m:
            block = dot3_narrow(split(a_ref[p, top:, here]), split(wt))
            left = split(block)
            right = split(jnp.transpose(block))
            for h in range(2):
                l_ref[keep + h, top:, here] = left[h]
                lt_ref[h, at, top:] = right[h]
        if odd == 0:
            a_ref[p, top:, B:] -= dot3_narrow(left, [r[:, :B] for r in right])
            d_ref[1] = wt
            d_ref[2] = jnp.transpose(block[:B])
            d_ref[0] = a_ref[p, top:top + B, B:]
        else:
            first = d_ref[1]
            inner = dot3_narrow(split(d_ref[2]), split(wt))
            corner = -dot3_narrow(split(first), split(inner))
            upper = jnp.concatenate([first, corner], axis=1)
            lower = jnp.concatenate([jnp.zeros_like(wt), wt], axis=1)
            wt_ref[0], wt_ref[1] = split(jnp.concatenate([upper, lower], axis=0))
            if top < m:
                right = [lt_ref[h, p * S:top, top:top + S] for h in range(2)]
                a_ref[p + 1, top:, :] -= dot3((l_ref[keep, top:, :], l_ref[keep + 1, top:, :]), right)
                d_ref[0] = a_ref[p + 1, top:top + B, :B]

    for p in range(stages):
        def stage(odd, carry, p=p):
            pieces = []
            for j in range(p + 1, stages):
                if p:
                    pieces.append(functools.partial(core_piece, p - 1, j, odd))
            for block in range(half // ROWS):
                at = pl.multiple_of(odd * half + block * ROWS, ROWS)
                if p == 0:
                    pieces += [functools.partial(cross_piece, j, at) for j in range(stages)]
                else:
                    pieces.append(functools.partial(raw_piece, p - 1, at))
                    pieces += [functools.partial(update_piece, p - 1, j, at) for j in range(p, stages)]
            done = 0
            for k in factor_block(d_ref.at[0], c_ref, sub, lane):
                until = -(-len(pieces) * (k + 1) // 14)
                for piece in pieces[done:until]:
                    piece()
                done = max(done, until)
            for o in range(2):
                pl.when(odd == o)(functools.partial(finish, p, o))
            if p:
                copy(p - 1, odd).start()
            return carry

        lax.fori_loop(0, 2, stage, 0)

    def last(odd, carry):
        for block in range(half // ROWS):
            raw_piece(stages - 1, pl.multiple_of(odd * half + block * ROWS, ROWS))
        copy(stages - 1, odd).start()
        return carry

    lax.fori_loop(0, 2, last, 0)
    for p in range(stages):
        for odd in range(2):
            copy(p, odd).wait()


def exchange(x, bit):
    dev = lax.axis_size("dev")
    axis, flip = ("dev", bit) if bit < dev else ("grp", bit // dev)
    size = lax.axis_size(axis)
    return lax.ppermute(x, axis, [(k, k ^ flip) for k in range(size)])


def shards(points, ridge, landmark_ids):
    count, width = points.shape
    m = landmark_ids.shape[0]
    devices = lax.axis_size(AXES)
    me = lax.axis_index(AXES)
    mean = m / devices
    cap = min(m, 16 * math.ceil((mean + 5.6 * math.sqrt(mean)) / 16))
    bits = [1 << b for b in range(devices.bit_length() - 1)]
    order = bits[1:] + bits[:1]

    bounds = jnp.sum(landmark_ids[None, :] < (jnp.arange(devices + 1) * count)[:, None], axis=1, dtype=jnp.int32)
    low = bounds[:-1]
    fits = jnp.max(bounds[1:] - low) <= cap

    def packed(points, ids):
        mine = lax.dynamic_slice(jnp.pad(ids, (0, cap)), (low[me],), (cap,))
        rows = points[jnp.clip(mine - me * count, 0, count - 1)]
        for bit in order:
            rows = jnp.concatenate([rows, exchange(rows, bit)], axis=0)
        far = jnp.arange(devices, dtype=jnp.int32) ^ me
        place = jnp.zeros_like(far)
        for k, bit in enumerate(order):
            place = place + jnp.where((far & bit) != 0, 1 << k, 0)
        return rows, place, low

    def summed(points, ids):
        offset = ids - me * count
        inside = (offset >= 0) & (offset < count)
        picked = points[jnp.clip(offset, 0, count - 1)]
        rows = lax.psum(jnp.where(inside[:, None], picked.astype(jnp.float32), 0.0), AXES).astype(points.dtype)
        rows = jnp.pad(rows, ((0, max(0, devices * cap - m)), (0, 0)))
        place = jnp.arange(devices, dtype=jnp.int32) % (m // cap)
        return rows, place, place * cap

    rows, src, dst = lax.cond(fits, packed, summed, points, landmark_ids)

    vmem = pl.BlockSpec(memory_space=pltpu.VMEM)
    raw, stat = pl.pallas_call(
        kernel,
        grid_spec=pltpu.PrefetchScalarGridSpec(
            num_scalar_prefetch=2,
            grid=(),
            in_specs=[vmem, vmem, vmem],
            out_specs=[pl.BlockSpec(memory_space=pl.ANY), vmem],
            scratch_shapes=[
                pltpu.VMEM((m, width), jnp.bfloat16),
                pltpu.VMEM((width // B, m + cap, B), jnp.float32),
                pltpu.VMEM((8, m), jnp.float32),
                pltpu.VMEM((m // S, m, S), jnp.float32),
                pltpu.VMEM((3, B, B), jnp.float32),
                pltpu.VMEM((B, B), jnp.float32),
                pltpu.VMEM((4, m, S), jnp.bfloat16),
                pltpu.VMEM((2, m, m), jnp.bfloat16),
                pltpu.VMEM((2, S, S), jnp.bfloat16),
                pltpu.VMEM((m // S, count, S), jnp.float32),
                pltpu.VMEM((2, count, S), jnp.bfloat16),
                pltpu.SemaphoreType.DMA((m // S, 2)),
            ],
        ),
        out_shape=(jax.ShapeDtypeStruct((count, m), jnp.float32), jax.ShapeDtypeStruct((8, m), jnp.float32)),
        compiler_params=pltpu.CompilerParams(vmem_limit_bytes=60 << 20),
        name="nystrom",
    )(src, dst, rows, points, ridge[None, :])

    stat = stat[:2]
    total = count
    for bit in bits:
        other = exchange(stat, bit)
        delta = other[0] - stat[0]
        stat = jnp.stack([0.5 * (stat[0] + other[0]), stat[1] + other[1] + jnp.square(delta) * (0.5 * total)])
        total *= 2
    var = stat[1] / total
    return ((raw - stat[0][None, :]) / jnp.sqrt(var + 1e-05)[None, :]).astype(jnp.bfloat16)


def solution(mesh):
    placed = (P(AXES, None), P(), P())
    return jax.shard_map(shards, mesh=mesh, in_specs=placed, out_specs=P(AXES, None), check_vma=False)
```

```python
import functools
import math

import jax
import jax.numpy as jnp
from jax import lax
from jax.experimental import pallas as pl
from jax.experimental.pallas import tpu as pltpu
from jax.sharding import PartitionSpec as P

AXES = ("grp", "dev")
B = 128
S = 256
ROWS = 512


def split(x):
    hi = x.astype(jnp.bfloat16)
    return hi, (x - hi.astype(jnp.float32)).astype(jnp.bfloat16)


def dot(left, right, dims=((1,), (0,))):
    return lax.dot_general(left, right, (dims, ((), ())), preferred_element_type=jnp.float32)


def dot_nt(left, right):
    return dot(left, right, ((1,), (1,)))


def dot3(left, right):
    return dot(left[0], right[0]) + dot(left[1], right[0]) + dot(left[0], right[1])


def dot3_narrow(left, right):
    left = jnp.concatenate([left[0], left[1], left[0]], axis=1)
    right = jnp.concatenate([right[0], right[0], right[1]], axis=0)
    return dot(left, right)


def factor_block(d_ref, c_ref, sub, lane):
    n = B // 8
    rows = [d_ref[8 * t:8 * t + 8, :] for t in range(n)]

    def column(t, at):
        return jnp.broadcast_to(rows[t][:, at:at + 1], (8, B))

    def spread(at):
        return jnp.broadcast_to(c_ref[at:at + 1, :], (8, B))

    ahead = [column(0, b) for b in range(8)]
    for k in range(n):
        first = 8 * k
        base = (k % 2) * 128
        follow = k + 1 < n
        for b in range(8):
            c_ref[base + 8 * b:base + 8 * b + 8, :] = ahead[b]
        s = {(a, b): spread(base + 8 * b + a) for b in range(8) for a in range(b + 1)}
        if follow:
            z = [column(k + 1, first + j) for j in range(8)]
            ahead = [column(k + 1, first + 8 + b) for b in range(8)]
            acc = rows[k + 1]
        below = {t: [column(t, first + j) for j in range(8)] for t in range(k + 2, n)}
        pivot = (lane >= first) & (lane < first + 8)
        start = jnp.where(pivot, (lane - first == sub).astype(jnp.float32), rows[k])
        y = [jnp.broadcast_to(start[i:i + 1, :], (8, B)) for i in range(8)]
        if follow:
            acc = jnp.where(pivot, 0.0, acc)
        inv = []
        for j in range(8):
            r = lax.rsqrt(s[(j, j)])
            inv.append(r)
            for b in range(j + 1, 8):
                s[(j, b)] = s[(j, b)] * r
            y[j] = y[j] * r
            if follow:
                z[j] = z[j] * r
                acc = acc - z[j] * y[j]
                at = base + 64 + 8 * j
                c_ref[at:at + 8, :] = z[j]
                for b in range(8):
                    ahead[b] = ahead[b] - z[j] * spread(at + b)
            for b in range(j + 1, 8):
                for a in range(j + 1, b + 1):
                    s[(a, b)] = s[(a, b)] - s[(j, a)] * s[(j, b)]
            for b in range(j + 1, 8):
                y[b] = y[b] - s[(j, b)] * y[j]
                if follow:
                    z[b] = z[b] - s[(j, b)] * z[j]
        w = y[7]
        for i in range(7):
            w = jnp.where(sub == i, y[i], w)
        d_ref[first:first + 8, :] = jnp.where(lane < first + 8, w, 0.0)
        if follow:
            rows[k + 1] = acc
        if k + 2 < n:
            q = [None] * 8
            for j in range(7, -1, -1):
                v = y[j]
                for i in range(j + 1, 8):
                    v = v - s[(j, i)] * q[i]
                q[j] = v * inv[j]
            for t in range(k + 2, n):
                v = jnp.where(pivot, 0.0, rows[t])
                for j in range(8):
                    v = v - below[t][j] * q[j]
                rows[t] = v
        yield k


def square_sums(x):
    hi, lo = split(jnp.square(x.astype(jnp.float32)))
    both = jnp.concatenate([hi, lo], axis=1)
    return dot_nt(jnp.ones((8, both.shape[1]), jnp.bfloat16), both), dot_nt(both, jnp.ones((B, both.shape[1]), jnp.bfloat16))


def wide(x):
    return jnp.concatenate([x] * (S // B), axis=1)


def kernel(src_ref, dst_ref, rows_ref, points_ref, ridge_ref, x_ref, stat_ref,
           marks_ref, packed_ref, along_ref, a_ref, d_ref, c_ref, l_ref, lt_ref, wt_ref, r_ref):
    m, width = marks_ref.shape
    count = points_ref.shape[0]
    scale = 1.0 / (2.0 * width)
    cap = packed_ref.shape[1] - m
    stages = m // S
    half = count // 2
    sub = lax.broadcasted_iota(jnp.int32, (8, B), 0)
    lane = lax.broadcasted_iota(jnp.int32, (8, B), 1)

    def place(d, carry):
        rows = rows_ref[pl.ds(pl.multiple_of(src_ref[d] * cap, cap), cap), :].astype(jnp.float32)
        for c in range(width // B):
            packed_ref[c, pl.ds(dst_ref[d], cap), :] = rows[:, c * B:(c + 1) * B]
        return carry

    lax.fori_loop(0, src_ref.shape[0], place, 0)
    marks_ref[...] = jnp.concatenate([packed_ref[c, :m] for c in range(width // B)], axis=1).astype(jnp.bfloat16)
    marks = marks_ref[...]
    along, down = square_sums(marks)
    along_ref[...] = along
    down = wide(down)
    stat_ref[...] = jnp.zeros_like(stat_ref)
    row = lax.broadcasted_iota(jnp.int32, (S, S), 0)
    col = lax.broadcasted_iota(jnp.int32, (S, S), 1)
    for j in range(stages):
        here = slice(j * S, (j + 1) * S)
        inner = dot_nt(marks[j * S:], marks[here])
        a_ref[j, j * S:, :] = jnp.exp(-(down[j * S:] + along[0:1, here] - 2.0 * inner) * scale)
        a_ref[j, here, :] += jnp.where(row == col, ridge_ref[0:1, here], 0.0)
    d_ref[0] = a_ref[0, :B, :B]

    def cross_piece(j, at):
        here = slice(j * S, (j + 1) * S)
        rows = pl.ds(at, ROWS)
        points = points_ref[rows, :]
        _, down = square_sums(points)
        inner = dot_nt(points, marks_ref[here, :])
        x_ref[j, rows, :] = jnp.exp(-(wide(down) + along_ref[0:1, here] - 2.0 * inner) * scale)

    def raw_piece(p, at):
        here = slice(p * S, (p + 1) * S)
        rows = pl.ds(at, ROWS)
        raw = dot3(split(x_ref[p, rows, :]), (wt_ref[0], wt_ref[1]))
        x_ref[p, rows, :] = raw
        r_ref[0, rows, :], r_ref[1, rows, :] = split(raw)
        mean = jnp.mean(raw, axis=0, keepdims=True)
        spread = jnp.sum(jnp.square(raw - mean), axis=0, keepdims=True)
        before = jnp.asarray(at).astype(jnp.float32)
        share = ROWS / (before + ROWS)
        delta = mean - stat_ref[0:1, here]
        stat_ref[1:2, here] += spread + jnp.square(delta) * (before * share)
        stat_ref[0:1, here] += delta * share

    def update_piece(p, j, at):
        rows = pl.ds(at, ROWS)
        right = [lt_ref[h, p * S:(p + 1) * S, j * S:(j + 1) * S] for h in range(2)]
        x_ref[j, rows, :] -= dot3((r_ref[0, rows, :], r_ref[1, rows, :]), right)

    def core_piece(p, j, odd):
        size = (m - j * S) // 2
        rows = pl.ds(pl.multiple_of(j * S + odd * size, B), size)
        right = [lt_ref[h, p * S:(p + 1) * S, j * S:(j + 1) * S] for h in range(2)]
        keep = 2 * (p % 2)
        a_ref[j, rows, :] -= dot3((l_ref[keep, rows, :], l_ref[keep + 1, rows, :]), right)

    def finish(p, odd):
        top = p * S + (odd + 1) * B
        here = slice(odd * B, (odd + 1) * B)
        at = slice(p * S + odd * B, p * S + (odd + 1) * B)
        keep = 2 * (p % 2)
        wt = jnp.transpose(d_ref[0])
        if top < m:
            block = dot3_narrow(split(a_ref[p, top:, here]), split(wt))
            left = split(block)
            right = split(jnp.transpose(block))
            for h in range(2):
                l_ref[keep + h, top:, here] = left[h]
                lt_ref[h, at, top:] = right[h]
        if odd == 0:
            a_ref[p, top:, B:] -= dot3_narrow(left, [r[:, :B] for r in right])
            d_ref[1] = wt
            d_ref[2] = jnp.transpose(block[:B])
            d_ref[0] = a_ref[p, top:top + B, B:]
        else:
            first = d_ref[1]
            inner = dot3_narrow(split(d_ref[2]), split(wt))
            corner = -dot3_narrow(split(first), split(inner))
            upper = jnp.concatenate([first, corner], axis=1)
            lower = jnp.concatenate([jnp.zeros_like(wt), wt], axis=1)
            wt_ref[0], wt_ref[1] = split(jnp.concatenate([upper, lower], axis=0))
            if top < m:
                right = [lt_ref[h, p * S:top, top:top + S] for h in range(2)]
                a_ref[p + 1, top:, :] -= dot3((l_ref[keep, top:, :], l_ref[keep + 1, top:, :]), right)
                d_ref[0] = a_ref[p + 1, top:top + B, :B]

    for p in range(stages):
        def stage(odd, carry, p=p):
            pieces = []
            for j in range(p + 1, stages):
                if p:
                    pieces.append(functools.partial(core_piece, p - 1, j, odd))
            for block in range(half // ROWS):
                at = pl.multiple_of(odd * half + block * ROWS, ROWS)
                if p == 0:
                    pieces += [functools.partial(cross_piece, j, at) for j in range(stages)]
                else:
                    pieces.append(functools.partial(raw_piece, p - 1, at))
                    pieces += [functools.partial(update_piece, p - 1, j, at) for j in range(p, stages)]
            done = 0
            for k in factor_block(d_ref.at[0], c_ref, sub, lane):
                until = -(-len(pieces) * (k + 1) // 14)
                for piece in pieces[done:until]:
                    piece()
                done = max(done, until)
            for o in range(2):
                pl.when(odd == o)(functools.partial(finish, p, o))
            return carry

        lax.fori_loop(0, 2, stage, 0)

    def last(odd, carry):
        for block in range(half // ROWS):
            raw_piece(stages - 1, pl.multiple_of(odd * half + block * ROWS, ROWS))
        return carry

    lax.fori_loop(0, 2, last, 0)


def standardize(x_ref, shift_ref, gain_ref, out_ref):
    size = out_ref.shape[0]
    rows = pl.ds(pl.multiple_of(pl.program_id(0) * size, size), size)
    for p in range(x_ref.shape[0]):
        here = slice(p * S, (p + 1) * S)
        out_ref[:, here] = ((x_ref[p, rows, :] - shift_ref[:, here]) * gain_ref[:, here]).astype(out_ref.dtype)


def exchange(x, bit):
    dev = lax.axis_size("dev")
    axis, flip = ("dev", bit) if bit < dev else ("grp", bit // dev)
    size = lax.axis_size(axis)
    return lax.ppermute(x, axis, [(k, k ^ flip) for k in range(size)])


def shards(points, ridge, landmark_ids):
    count, width = points.shape
    m = landmark_ids.shape[0]
    devices = lax.axis_size(AXES)
    me = lax.axis_index(AXES)
    mean = m / devices
    cap = min(m, 16 * math.ceil((mean + 5.6 * math.sqrt(mean)) / 16))
    bits = [1 << b for b in range(devices.bit_length() - 1)]
    order = bits[1:] + bits[:1]

    bounds = jnp.sum(landmark_ids[None, :] < (jnp.arange(devices + 1) * count)[:, None], axis=1, dtype=jnp.int32)
    low = bounds[:-1]
    fits = jnp.max(bounds[1:] - low) <= cap

    def packed(points, ids):
        mine = lax.dynamic_slice(jnp.pad(ids, (0, cap)), (low[me],), (cap,))
        rows = points[jnp.clip(mine - me * count, 0, count - 1)]
        for bit in order:
            rows = jnp.concatenate([rows, exchange(rows, bit)], axis=0)
        far = jnp.arange(devices, dtype=jnp.int32) ^ me
        place = jnp.zeros_like(far)
        for k, bit in enumerate(order):
            place = place + jnp.where((far & bit) != 0, 1 << k, 0)
        return rows, place, low

    def summed(points, ids):
        offset = ids - me * count
        inside = (offset >= 0) & (offset < count)
        picked = points[jnp.clip(offset, 0, count - 1)]
        rows = lax.psum(jnp.where(inside[:, None], picked.astype(jnp.float32), 0.0), AXES).astype(points.dtype)
        rows = jnp.pad(rows, ((0, max(0, devices * cap - m)), (0, 0)))
        place = jnp.arange(devices, dtype=jnp.int32) % (m // cap)
        return rows, place, place * cap

    rows, src, dst = lax.cond(fits, packed, summed, points, landmark_ids)

    vmem = pl.BlockSpec(memory_space=pltpu.VMEM)
    raw, stat = pl.pallas_call(
        kernel,
        grid_spec=pltpu.PrefetchScalarGridSpec(
            num_scalar_prefetch=2,
            grid=(),
            in_specs=[vmem, vmem, vmem],
            out_specs=[vmem, vmem],
            scratch_shapes=[
                pltpu.VMEM((m, width), jnp.bfloat16),
                pltpu.VMEM((width // B, m + cap, B), jnp.float32),
                pltpu.VMEM((8, m), jnp.float32),
                pltpu.VMEM((m // S, m, S), jnp.float32),
                pltpu.VMEM((3, B, B), jnp.float32),
                pltpu.VMEM((2 * B, B), jnp.float32),
                pltpu.VMEM((4, m, S), jnp.bfloat16),
                pltpu.VMEM((2, m, m), jnp.bfloat16),
                pltpu.VMEM((2, S, S), jnp.bfloat16),
                pltpu.VMEM((2, count, S), jnp.bfloat16),
            ],
        ),
        out_shape=(pltpu.VMEM((m // S, count, S), jnp.float32), jax.ShapeDtypeStruct((2, m), jnp.float32)),
        compiler_params=pltpu.CompilerParams(vmem_limit_bytes=40 << 20),
        name="nystrom",
    )(src, dst, rows, points, ridge[None, :])

    total = count
    for bit in bits:
        other = exchange(stat, bit)
        delta = other[0] - stat[0]
        stat = jnp.stack([0.5 * (stat[0] + other[0]), stat[1] + other[1] + jnp.square(delta) * (0.5 * total)])
        total *= 2
    gain = 1.0 / jnp.sqrt(stat[1:2] / total + 1e-05)
    vector = pl.BlockSpec((1, m), lambda i: (0, 0))
    return pl.pallas_call(
        standardize,
        grid=(count // 256,),
        in_specs=[vmem, vector, vector],
        out_specs=pl.BlockSpec((256, m), lambda i: (i, 0)),
        out_shape=jax.ShapeDtypeStruct((count, m), jnp.bfloat16),
        compiler_params=pltpu.CompilerParams(vmem_limit_bytes=16 << 20, dimension_semantics=("arbitrary",)),
        name="standardize",
    )(raw, stat[0:1], gain)


def solution(mesh):
    placed = (P(AXES, None), P(), P())
    return jax.shard_map(shards, mesh=mesh, in_specs=placed, out_specs=P(AXES, None), check_vma=False)
```

```python
import functools
import math

import jax
import jax.numpy as jnp
from jax import lax
from jax.experimental import pallas as pl
from jax.experimental.pallas import tpu as pltpu
from jax.sharding import PartitionSpec as P

AXES = ("grp", "dev")
B = 128
S = 256
ROWS = 512


def split(x):
    hi = x.astype(jnp.bfloat16)
    return hi, (x - hi.astype(jnp.float32)).astype(jnp.bfloat16)


def dot(left, right, dims=((1,), (0,))):
    return lax.dot_general(left, right, (dims, ((), ())), preferred_element_type=jnp.float32)


def dot_nt(left, right):
    return dot(left, right, ((1,), (1,)))


def dot3(left, right):
    return dot(left[0], right[0]) + dot(left[1], right[0]) + dot(left[0], right[1])


def dot3_narrow(left, right):
    left = jnp.concatenate([left[0], left[1], left[0]], axis=1)
    right = jnp.concatenate([right[0], right[0], right[1]], axis=0)
    return dot(left, right)


def factor_block(d_ref, c_ref, sub, lane):
    n = B // 8
    rows = [d_ref[8 * t:8 * t + 8, :] for t in range(n)]

    def column(t, at):
        return jnp.broadcast_to(rows[t][:, at:at + 1], (8, B))

    def spread(at):
        return jnp.broadcast_to(c_ref[at:at + 1, :], (8, B))

    ahead = [column(0, b) for b in range(8)]
    for k in range(n):
        first = 8 * k
        base = (k % 2) * 128
        follow = k + 1 < n
        for b in range(8):
            c_ref[base + 8 * b:base + 8 * b + 8, :] = ahead[b]
        s = {(a, b): spread(base + 8 * b + a) for b in range(8) for a in range(b + 1)}
        if follow:
            z = [column(k + 1, first + j) for j in range(8)]
            ahead = [column(k + 1, first + 8 + b) for b in range(8)]
            acc = rows[k + 1]
        below = {t: [column(t, first + j) for j in range(8)] for t in range(k + 2, n)}
        pivot = (lane >= first) & (lane < first + 8)
        start = jnp.where(pivot, (lane - first == sub).astype(jnp.float32), rows[k])
        y = [jnp.broadcast_to(start[i:i + 1, :], (8, B)) for i in range(8)]
        if follow:
            acc = jnp.where(pivot, 0.0, acc)
        inv = []
        for j in range(8):
            r = lax.rsqrt(s[(j, j)])
            inv.append(r)
            for b in range(j + 1, 8):
                s[(j, b)] = s[(j, b)] * r
            y[j] = y[j] * r
            if follow:
                z[j] = z[j] * r
                acc = acc - z[j] * y[j]
                at = base + 64 + 8 * j
                c_ref[at:at + 8, :] = z[j]
                for b in range(8):
                    ahead[b] = ahead[b] - z[j] * spread(at + b)
            for b in range(j + 1, 8):
                for a in range(j + 1, b + 1):
                    s[(a, b)] = s[(a, b)] - s[(j, a)] * s[(j, b)]
            for b in range(j + 1, 8):
                y[b] = y[b] - s[(j, b)] * y[j]
                if follow:
                    z[b] = z[b] - s[(j, b)] * z[j]
        w = y[7]
        for i in range(7):
            w = jnp.where(sub == i, y[i], w)
        d_ref[first:first + 8, :] = jnp.where(lane < first + 8, w, 0.0)
        if follow:
            rows[k + 1] = acc
        if k + 2 < n:
            q = [None] * 8
            for j in range(7, -1, -1):
                v = y[j]
                for i in range(j + 1, 8):
                    v = v - s[(j, i)] * q[i]
                q[j] = v * inv[j]
            for t in range(k + 2, n):
                v = jnp.where(pivot, 0.0, rows[t])
                for j in range(8):
                    v = v - below[t][j] * q[j]
                rows[t] = v
        yield k


def square_sums(x):
    hi, lo = split(jnp.square(x.astype(jnp.float32)))
    both = jnp.concatenate([hi, lo], axis=1)
    return dot_nt(jnp.ones((8, both.shape[1]), jnp.bfloat16), both), dot_nt(both, jnp.ones((B, both.shape[1]), jnp.bfloat16))


def wide(x):
    return jnp.concatenate([x] * (S // B), axis=1)


def kernel(order, info_ref, low_ref, own_ref, other_ref, points_ref, ridge_ref, x_ref, stat_ref,
           marks_ref, packed_ref, along_ref, a_ref, d_ref, c_ref, l_ref, lt_ref, wt_ref, r_ref):
    m, width = marks_ref.shape
    count = points_ref.shape[0]
    scale = 1.0 / (2.0 * width)
    cap = packed_ref.shape[1] - m
    stages = m // S
    half = count // 2
    sub = lax.broadcasted_iota(jnp.int32, (8, B), 0)
    lane = lax.broadcasted_iota(jnp.int32, (8, B), 1)

    half_rows = own_ref.shape[0]

    def place(d, carry):
        packed = info_ref[0] != 0
        far = d ^ info_ref[1]
        block = 0
        for k, bit in enumerate(order):
            block = block + jnp.where((far & bit) != 0, 1 << k, 0)
        plain = d % (m // cap)
        source = jnp.where(packed, block, plain) * cap
        target = jnp.where(packed, low_ref[d], plain * cap)
        at = pl.ds(pl.multiple_of(source % half_rows, cap), cap)
        rows = jnp.where(source < half_rows, own_ref[at, :], other_ref[at, :]).astype(jnp.float32)
        for c in range(width // B):
            packed_ref[c, pl.ds(target, cap), :] = rows[:, c * B:(c + 1) * B]
        return carry

    lax.fori_loop(0, 1 << len(order), place, 0)
    marks_ref[...] = jnp.concatenate([packed_ref[c, :m] for c in range(width // B)], axis=1).astype(jnp.bfloat16)
    marks = marks_ref[...]
    along, down = square_sums(marks)
    along_ref[...] = along
    down = wide(down)
    stat_ref[...] = jnp.zeros_like(stat_ref)
    row = lax.broadcasted_iota(jnp.int32, (S, S), 0)
    col = lax.broadcasted_iota(jnp.int32, (S, S), 1)
    for j in range(stages):
        here = slice(j * S, (j + 1) * S)
        inner = dot_nt(marks[j * S:], marks[here])
        a_ref[j, j * S:, :] = jnp.exp(-(down[j * S:] + along[0:1, here] - 2.0 * inner) * scale)
        a_ref[j, here, :] += jnp.where(row == col, ridge_ref[0:1, here], 0.0)
    d_ref[0] = a_ref[0, :B, :B]

    def cross_piece(j, at):
        here = slice(j * S, (j + 1) * S)
        rows = pl.ds(at, ROWS)
        points = points_ref[rows, :]
        _, down = square_sums(points)
        inner = dot_nt(points, marks_ref[here, :])
        x_ref[j, rows, :] = jnp.exp(-(wide(down) + along_ref[0:1, here] - 2.0 * inner) * scale)

    def raw_piece(p, at):
        here = slice(p * S, (p + 1) * S)
        rows = pl.ds(at, ROWS)
        raw = dot3(split(x_ref[p, rows, :]), (wt_ref[0], wt_ref[1]))
        x_ref[p, rows, :] = raw
        r_ref[0, rows, :], r_ref[1, rows, :] = split(raw)
        mean = jnp.mean(raw, axis=0, keepdims=True)
        spread = jnp.sum(jnp.square(raw - mean), axis=0, keepdims=True)
        before = jnp.asarray(at).astype(jnp.float32)
        share = ROWS / (before + ROWS)
        delta = mean - stat_ref[0:1, here]
        stat_ref[1:2, here] += spread + jnp.square(delta) * (before * share)
        stat_ref[0:1, here] += delta * share

    def update_piece(p, j, at):
        rows = pl.ds(at, ROWS)
        right = [lt_ref[h, p * S:(p + 1) * S, j * S:(j + 1) * S] for h in range(2)]
        x_ref[j, rows, :] -= dot3((r_ref[0, rows, :], r_ref[1, rows, :]), right)

    def core_piece(p, j, odd):
        size = (m - j * S) // 2
        rows = pl.ds(pl.multiple_of(j * S + odd * size, B), size)
        right = [lt_ref[h, p * S:(p + 1) * S, j * S:(j + 1) * S] for h in range(2)]
        keep = 2 * (p % 2)
        a_ref[j, rows, :] -= dot3((l_ref[keep, rows, :], l_ref[keep + 1, rows, :]), right)

    def finish(p, odd):
        top = p * S + (odd + 1) * B
        here = slice(odd * B, (odd + 1) * B)
        at = slice(p * S + odd * B, p * S + (odd + 1) * B)
        keep = 2 * (p % 2)
        wt = jnp.transpose(d_ref[0])
        if top < m:
            block = dot3_narrow(split(a_ref[p, top:, here]), split(wt))
            left = split(block)
            right = split(jnp.transpose(block))
            for h in range(2):
                l_ref[keep + h, top:, here] = left[h]
                lt_ref[h, at, top:] = right[h]
        if odd == 0:
            a_ref[p, top:, B:] -= dot3_narrow(left, [r[:, :B] for r in right])
            d_ref[1] = wt
            d_ref[2] = jnp.transpose(block[:B])
            d_ref[0] = a_ref[p, top:top + B, B:]
        else:
            first = d_ref[1]
            inner = dot3_narrow(split(d_ref[2]), split(wt))
            corner = -dot3_narrow(split(first), split(inner))
            upper = jnp.concatenate([first, corner], axis=1)
            lower = jnp.concatenate([jnp.zeros_like(wt), wt], axis=1)
            wt_ref[0], wt_ref[1] = split(jnp.concatenate([upper, lower], axis=0))
            if top < m:
                right = [lt_ref[h, p * S:top, top:top + S] for h in range(2)]
                a_ref[p + 1, top:, :] -= dot3((l_ref[keep, top:, :], l_ref[keep + 1, top:, :]), right)
                d_ref[0] = a_ref[p + 1, top:top + B, :B]

    for p in range(stages):
        def stage(odd, carry, p=p):
            pieces = []
            for j in range(p + 1, stages):
                if p:
                    pieces.append(functools.partial(core_piece, p - 1, j, odd))
            for block in range(half // ROWS):
                at = pl.multiple_of(odd * half + block * ROWS, ROWS)
                if p == 0:
                    pieces += [functools.partial(cross_piece, j, at) for j in range(stages)]
                else:
                    pieces.append(functools.partial(raw_piece, p - 1, at))
                    pieces += [functools.partial(update_piece, p - 1, j, at) for j in range(p, stages)]
            done = 0
            for k in factor_block(d_ref.at[0], c_ref, sub, lane):
                until = -(-len(pieces) * (k + 1) // 14)
                for piece in pieces[done:until]:
                    piece()
                done = max(done, until)
            for o in range(2):
                pl.when(odd == o)(functools.partial(finish, p, o))
            return carry

        lax.fori_loop(0, 2, stage, 0)

    def last(odd, carry):
        for block in range(half // ROWS):
            raw_piece(stages - 1, pl.multiple_of(odd * half + block * ROWS, ROWS))
        return carry

    lax.fori_loop(0, 2, last, 0)


def standardize(x_ref, shift_ref, gain_ref, out_ref):
    size = out_ref.shape[0]
    rows = pl.ds(pl.multiple_of(pl.program_id(0) * size, size), size)
    for p in range(x_ref.shape[0]):
        here = slice(p * S, (p + 1) * S)
        out_ref[:, here] = ((x_ref[p, rows, :] - shift_ref[:, here]) * gain_ref[:, here]).astype(out_ref.dtype)


def pack(devices, me_ref, ids_ref, line_ref, points_ref, rows_ref, low_ref, most_ref):
    cap = rows_ref.shape[0]
    count = points_ref.shape[0]
    m = ids_ref.shape[0]
    start = me_ref[0] * count

    def search(_, bounds):
        low, high = bounds
        middle = (low + high) // 2
        inside = (low < high) & (ids_ref[jnp.minimum(middle, m - 1)] < start)
        return jnp.where(inside, middle + 1, low), jnp.where(inside, high, jnp.where(low < high, middle, high))

    first, _ = lax.fori_loop(0, m.bit_length(), search, (jnp.int32(0), jnp.int32(m)))
    sub = lax.broadcasted_iota(jnp.int32, (8, B), 0)
    groups = []
    for g in range(cap // 8):
        slots = jnp.zeros((8, B), jnp.int32)
        for i in range(8):
            slots = jnp.where(sub == i, ids_ref[jnp.minimum(first + 8 * g + i, m - 1)] - start, slots)
        groups.append(slots)
    slots = jnp.concatenate(groups, axis=0)
    lane = lax.broadcasted_iota(jnp.int32, (cap, B), 1)
    picks = [(slots == lane + c * B).astype(jnp.float32).astype(jnp.bfloat16) for c in range(count // B)]
    rows_ref[...] = dot(jnp.concatenate(picks, axis=1), points_ref[...]).astype(rows_ref.dtype)
    size = low_ref.shape[1]
    device = lax.broadcasted_iota(jnp.int32, (size, m), 0)
    line = jnp.broadcast_to(line_ref[...], (size, m))
    ones = jnp.ones((8, m), jnp.bfloat16)
    low = dot_nt(ones, (line < device * count).astype(jnp.float32).astype(jnp.bfloat16))
    high = dot_nt(ones, (line < (device + 1) * count).astype(jnp.float32).astype(jnp.bfloat16))
    low_ref[...] = low[0:1].astype(jnp.int32)
    most_ref[...] = jnp.broadcast_to(jnp.max(high - low, axis=1, keepdims=True)[0:1], most_ref.shape).astype(jnp.int32)


def exchange(x, bit):
    dev = lax.axis_size("dev")
    axis, flip = ("dev", bit) if bit < dev else ("grp", bit // dev)
    size = lax.axis_size(axis)
    return lax.ppermute(x, axis, [(k, k ^ flip) for k in range(size)])


def shards(points, ridge, landmark_ids):
    count, width = points.shape
    m = landmark_ids.shape[0]
    devices = lax.axis_size(AXES)
    me = lax.axis_index(AXES)
    mean = m / devices
    cap = min(m, 16 * math.ceil((mean + 5.6 * math.sqrt(mean)) / 16))
    bits = [1 << b for b in range(devices.bit_length() - 1)]
    near = [bit for bit in bits[1:] if bit < lax.axis_size("dev")]
    far = [bit for bit in bits[1:] if bit >= lax.axis_size("dev")]
    order = (*near, *far, bits[0])
    vmem = pl.BlockSpec(memory_space=pltpu.VMEM)
    table = -(-devices // B) * B

    rows, low, most = pl.pallas_call(
        functools.partial(pack, devices),
        grid_spec=pltpu.PrefetchScalarGridSpec(
            num_scalar_prefetch=2, grid=(), in_specs=[vmem, vmem], out_specs=[vmem, vmem, vmem],
        ),
        out_shape=(
            jax.ShapeDtypeStruct((cap, width), points.dtype),
            jax.ShapeDtypeStruct((1, table), jnp.int32),
            jax.ShapeDtypeStruct((1, B), jnp.int32),
        ),
        compiler_params=pltpu.CompilerParams(vmem_limit_bytes=16 << 20),
        name="pack",
    )(me[None], landmark_ids, landmark_ids[None, :], points)
    fits = most[0, 0] <= cap

    def packed(rows, points, ids):
        for some in (near, far):
            for at in range(0, len(some), 2):
                pair = some[at:at + 2]
                moves = pair if len(pair) == 1 else (pair[0], pair[1], pair[0] | pair[1])
                rows = jnp.concatenate([rows, *(exchange(rows, move) for move in moves)], axis=0)
        return rows, exchange(rows, bits[0])

    def summed(rows, points, ids):
        offset = ids - me * count
        inside = (offset >= 0) & (offset < count)
        picked = points[jnp.clip(offset, 0, count - 1)]
        rows = lax.psum(jnp.where(inside[:, None], picked.astype(jnp.float32), 0.0), AXES).astype(points.dtype)
        rows = jnp.pad(rows, ((0, devices * cap - m), (0, 0)))
        return rows[:devices * cap // 2], rows[devices * cap // 2:]

    own, other = lax.cond(fits, packed, summed, rows, points, landmark_ids)
    info = jnp.stack([fits.astype(jnp.int32), me])

    raw, stat = pl.pallas_call(
        functools.partial(kernel, order),
        grid_spec=pltpu.PrefetchScalarGridSpec(
            num_scalar_prefetch=2,
            grid=(),
            in_specs=[vmem, vmem, vmem, vmem],
            out_specs=[vmem, vmem],
            scratch_shapes=[
                pltpu.VMEM((m, width), jnp.bfloat16),
                pltpu.VMEM((width // B, m + cap, B), jnp.float32),
                pltpu.VMEM((8, m), jnp.float32),
                pltpu.VMEM((m // S, m, S), jnp.float32),
                pltpu.VMEM((3, B, B), jnp.float32),
                pltpu.VMEM((2 * B, B), jnp.float32),
                pltpu.VMEM((4, m, S), jnp.bfloat16),
                pltpu.VMEM((2, m, m), jnp.bfloat16),
                pltpu.VMEM((2, S, S), jnp.bfloat16),
                pltpu.VMEM((2, count, S), jnp.bfloat16),
            ],
        ),
        out_shape=(pltpu.VMEM((m // S, count, S), jnp.float32), jax.ShapeDtypeStruct((2, m), jnp.float32)),
        compiler_params=pltpu.CompilerParams(vmem_limit_bytes=40 << 20),
        name="nystrom",
    )(info, low[0], own, other, points, ridge[None, :])

    total = count
    for bit in bits:
        other = exchange(stat, bit)
        delta = other[0] - stat[0]
        stat = jnp.stack([0.5 * (stat[0] + other[0]), stat[1] + other[1] + jnp.square(delta) * (0.5 * total)])
        total *= 2
    gain = 1.0 / jnp.sqrt(stat[1:2] / total + 1e-05)
    vector = pl.BlockSpec((1, m), lambda i: (0, 0))
    return pl.pallas_call(
        standardize,
        grid=(count // 256,),
        in_specs=[vmem, vector, vector],
        out_specs=pl.BlockSpec((256, m), lambda i: (i, 0)),
        out_shape=jax.ShapeDtypeStruct((count, m), jnp.bfloat16),
        compiler_params=pltpu.CompilerParams(vmem_limit_bytes=16 << 20, dimension_semantics=("arbitrary",)),
        name="standardize",
    )(raw, stat[0:1], gain)


def solution(mesh):
    placed = (P(AXES, None), P(), P())
    return jax.shard_map(shards, mesh=mesh, in_specs=placed, out_specs=P(AXES, None), check_vma=False)
```

```python
import functools
import math

import jax
import jax.numpy as jnp
from jax import lax
from jax.experimental import pallas as pl
from jax.experimental.pallas import tpu as pltpu
from jax.sharding import PartitionSpec as P

AXES = ("grp", "dev")
B = 128
S = 256
ROWS = 512


def split(x):
    hi = x.astype(jnp.bfloat16)
    return hi, (x - hi.astype(jnp.float32)).astype(jnp.bfloat16)


def dot(left, right, dims=((1,), (0,))):
    return lax.dot_general(left, right, (dims, ((), ())), preferred_element_type=jnp.float32)


def dot_nt(left, right):
    return dot(left, right, ((1,), (1,)))


def dot3(left, right):
    return dot(left[0], right[0]) + dot(left[1], right[0]) + dot(left[0], right[1])


def dot3_narrow(left, right):
    left = jnp.concatenate([left[0], left[1], left[0]], axis=1)
    right = jnp.concatenate([right[0], right[0], right[1]], axis=0)
    return dot(left, right)


def factor_block(d_ref, c_ref, sub, lane):
    n = B // 8
    rows = [d_ref[8 * t:8 * t + 8, :] for t in range(n)]

    def column(t, at):
        return jnp.broadcast_to(rows[t][:, at:at + 1], (8, B))

    def spread(at):
        return jnp.broadcast_to(c_ref[at:at + 1, :], (8, B))

    ahead = [column(0, b) for b in range(8)]
    for k in range(n):
        first = 8 * k
        base = (k % 2) * 128
        follow = k + 1 < n
        for b in range(8):
            c_ref[base + 8 * b:base + 8 * b + 8, :] = ahead[b]
        s = {(a, b): spread(base + 8 * b + a) for b in range(8) for a in range(b + 1)}
        if follow:
            z = [column(k + 1, first + j) for j in range(8)]
            ahead = [column(k + 1, first + 8 + b) for b in range(8)]
            acc = rows[k + 1]
        below = {t: [column(t, first + j) for j in range(8)] for t in range(k + 2, n)}
        pivot = (lane >= first) & (lane < first + 8)
        start = jnp.where(pivot, (lane - first == sub).astype(jnp.float32), rows[k])
        y = [jnp.broadcast_to(start[i:i + 1, :], (8, B)) for i in range(8)]
        if follow:
            acc = jnp.where(pivot, 0.0, acc)
        inv = []
        for j in range(8):
            r = lax.rsqrt(s[(j, j)])
            inv.append(r)
            for b in range(j + 1, 8):
                s[(j, b)] = s[(j, b)] * r
            y[j] = y[j] * r
            if follow:
                z[j] = z[j] * r
                acc = acc - z[j] * y[j]
                at = base + 64 + 8 * j
                c_ref[at:at + 8, :] = z[j]
                for b in range(8):
                    ahead[b] = ahead[b] - z[j] * spread(at + b)
            for b in range(j + 1, 8):
                for a in range(j + 1, b + 1):
                    s[(a, b)] = s[(a, b)] - s[(j, a)] * s[(j, b)]
            for b in range(j + 1, 8):
                y[b] = y[b] - s[(j, b)] * y[j]
                if follow:
                    z[b] = z[b] - s[(j, b)] * z[j]
        w = y[7]
        for i in range(7):
            w = jnp.where(sub == i, y[i], w)
        d_ref[first:first + 8, :] = jnp.where(lane < first + 8, w, 0.0)
        if follow:
            rows[k + 1] = acc
        if k + 2 < n:
            q = [None] * 8
            for j in range(7, -1, -1):
                v = y[j]
                for i in range(j + 1, 8):
                    v = v - s[(j, i)] * q[i]
                q[j] = v * inv[j]
            for t in range(k + 2, n):
                v = jnp.where(pivot, 0.0, rows[t])
                for j in range(8):
                    v = v - below[t][j] * q[j]
                rows[t] = v
        yield k


def square_sums(x):
    hi, lo = split(jnp.square(x.astype(jnp.float32)))
    both = jnp.concatenate([hi, lo], axis=1)
    return dot_nt(jnp.ones((8, both.shape[1]), jnp.bfloat16), both), dot_nt(both, jnp.ones((B, both.shape[1]), jnp.bfloat16))


def wide(x):
    return jnp.concatenate([x] * (S // B), axis=1)


def kernel(order, info_ref, low_ref, *refs):
    (*piece_refs, points_ref, ridge_ref, x_ref, stat_ref, marks_ref, rows_ref, packed_ref, along_ref, a_ref, d_ref,
     c_ref, l_ref, lt_ref, wt_ref, r_ref) = refs
    m, width = marks_ref.shape
    count = points_ref.shape[0]
    scale = 1.0 / (2.0 * width)
    cap = packed_ref.shape[1] - m
    stages = m // S
    half = count // 2
    sub = lax.broadcasted_iota(jnp.int32, (8, B), 0)
    lane = lax.broadcasted_iota(jnp.int32, (8, B), 1)

    size = piece_refs[0].shape[0]
    for k, piece_ref in enumerate(piece_refs):
        rows_ref[k * size:(k + 1) * size, :] = piece_ref[...]

    def place(d, carry):
        packed = info_ref[0] != 0
        far = d ^ info_ref[1]
        block = 0
        for k, bit in enumerate(order):
            block = block + jnp.where((far & bit) != 0, 1 << k, 0)
        plain = d % (m // cap)
        source = jnp.where(packed, block, plain) * cap
        target = jnp.where(packed, low_ref[d], plain * cap)
        rows = rows_ref[pl.ds(pl.multiple_of(source, cap), cap), :].astype(jnp.float32)
        for c in range(width // B):
            packed_ref[c, pl.ds(target, cap), :] = rows[:, c * B:(c + 1) * B]
        return carry

    lax.fori_loop(0, 1 << len(order), place, 0)
    marks_ref[...] = jnp.concatenate([packed_ref[c, :m] for c in range(width // B)], axis=1).astype(jnp.bfloat16)
    marks = marks_ref[...]
    along, down = square_sums(marks)
    along_ref[...] = along
    down = wide(down)
    stat_ref[...] = jnp.zeros_like(stat_ref)
    row = lax.broadcasted_iota(jnp.int32, (S, S), 0)
    col = lax.broadcasted_iota(jnp.int32, (S, S), 1)
    for j in range(stages):
        here = slice(j * S, (j + 1) * S)
        inner = dot_nt(marks[j * S:], marks[here])
        a_ref[j, j * S:, :] = jnp.exp(-(down[j * S:] + along[0:1, here] - 2.0 * inner) * scale)
        a_ref[j, here, :] += jnp.where(row == col, ridge_ref[0:1, here], 0.0)
    d_ref[0] = a_ref[0, :B, :B]

    def cross_piece(j, at):
        here = slice(j * S, (j + 1) * S)
        rows = pl.ds(at, ROWS)
        points = points_ref[rows, :]
        _, down = square_sums(points)
        inner = dot_nt(points, marks_ref[here, :])
        x_ref[j, rows, :] = jnp.exp(-(wide(down) + along_ref[0:1, here] - 2.0 * inner) * scale)

    def raw_piece(p, at):
        here = slice(p * S, (p + 1) * S)
        rows = pl.ds(at, ROWS)
        raw = dot3(split(x_ref[p, rows, :]), (wt_ref[0], wt_ref[1]))
        x_ref[p, rows, :] = raw
        keep = 2 * (p % 2)
        r_ref[keep, rows, :], r_ref[keep + 1, rows, :] = split(raw)
        mean = jnp.mean(raw, axis=0, keepdims=True)
        spread = jnp.sum(jnp.square(raw - mean), axis=0, keepdims=True)
        before = jnp.asarray(at).astype(jnp.float32)
        share = ROWS / (before + ROWS)
        delta = mean - stat_ref[0:1, here]
        stat_ref[1:2, here] += spread + jnp.square(delta) * (before * share)
        stat_ref[0:1, here] += delta * share

    def update_piece(p, j, at):
        rows = pl.ds(at, ROWS)
        right = [lt_ref[h, p * S:(p + 1) * S, j * S:(j + 1) * S] for h in range(2)]
        keep = 2 * (p % 2)
        x_ref[j, rows, :] -= dot3((r_ref[keep, rows, :], r_ref[keep + 1, rows, :]), right)

    def core_piece(p, j, odd):
        size = (m - j * S) // 2
        rows = pl.ds(pl.multiple_of(j * S + odd * size, B), size)
        right = [lt_ref[h, p * S:(p + 1) * S, j * S:(j + 1) * S] for h in range(2)]
        keep = 2 * (p % 2)
        a_ref[j, rows, :] -= dot3((l_ref[keep, rows, :], l_ref[keep + 1, rows, :]), right)

    def finish(p, odd):
        top = p * S + (odd + 1) * B
        here = slice(odd * B, (odd + 1) * B)
        at = slice(p * S + odd * B, p * S + (odd + 1) * B)
        keep = 2 * (p % 2)
        wt = jnp.transpose(d_ref[0])
        if top < m:
            block = dot3_narrow(split(a_ref[p, top:, here]), split(wt))
            left = split(block)
            right = split(jnp.transpose(block))
            for h in range(2):
                l_ref[keep + h, top:, here] = left[h]
                lt_ref[h, at, top:] = right[h]
        if odd == 0:
            a_ref[p, top:, B:] -= dot3_narrow(left, [r[:, :B] for r in right])
            d_ref[1] = wt
            d_ref[2] = jnp.transpose(block[:B])
            d_ref[0] = a_ref[p, top:top + B, B:]
        else:
            first = d_ref[1]
            inner = dot3_narrow(split(d_ref[2]), split(wt))
            corner = -dot3_narrow(split(first), split(inner))
            upper = jnp.concatenate([first, corner], axis=1)
            lower = jnp.concatenate([jnp.zeros_like(wt), wt], axis=1)
            wt_ref[0], wt_ref[1] = split(jnp.concatenate([upper, lower], axis=0))
            if top < m:
                right = [lt_ref[h, p * S:top, top:top + S] for h in range(2)]
                a_ref[p + 1, top:, :] -= dot3((l_ref[keep, top:, :], l_ref[keep + 1, top:, :]), right)
                d_ref[0] = a_ref[p + 1, top:top + B, :B]

    def turn(q, j):
        return q + 2 if q and j > q + 1 else min(max(j - 1, q + 1), q + 2)

    for p in range(stages):
        def stage(odd, carry, p=p):
            pieces = []
            for j in range(p + 1, stages):
                if p:
                    pieces.append(functools.partial(core_piece, p - 1, j, odd))
            for block in range(half // ROWS):
                at = pl.multiple_of(odd * half + block * ROWS, ROWS)
                if p:
                    pieces.append(functools.partial(raw_piece, p - 1, at))
                for j in range(stages):
                    if p == min(max(j - 1, 0), 2):
                        pieces.append(functools.partial(cross_piece, j, at))
                    pieces += [functools.partial(update_piece, q, j, at) for q in range(j) if p == turn(q, j)]
            done = 0
            for k in factor_block(d_ref.at[0], c_ref, sub, lane):
                until = -(-len(pieces) * (k + 1) // 14)
                for piece in pieces[done:until]:
                    piece()
                done = max(done, until)
            for o in range(2):
                pl.when(odd == o)(functools.partial(finish, p, o))
            return carry

        lax.fori_loop(0, 2, stage, 0)

    def last(odd, carry):
        for block in range(half // ROWS):
            raw_piece(stages - 1, pl.multiple_of(odd * half + block * ROWS, ROWS))
        return carry

    lax.fori_loop(0, 2, last, 0)


def standardize(x_ref, shift_ref, gain_ref, out_hbm, out_ref, sems):
    steps, size, _ = out_ref.shape

    def copy(k):
        return pltpu.make_async_copy(out_ref.at[k], out_hbm.at[k * size:(k + 1) * size, :], sems.at[k])

    for k in range(steps):
        for p in range(x_ref.shape[0]):
            here = slice(p * S, (p + 1) * S)
            x = x_ref[p, k * size:(k + 1) * size, :]
            out_ref[k, :, here] = ((x - shift_ref[:, here]) * gain_ref[:, here]).astype(out_ref.dtype)
        copy(k).start()
    for k in range(steps):
        copy(k).wait()


def pack(devices, me_ref, ids_ref, line_ref, points_ref, rows_ref, low_ref, most_ref, kept_ref):
    cap = rows_ref.shape[0]
    count = points_ref.shape[0]
    m = ids_ref.shape[0]
    kept_ref[...] = points_ref[...]
    start = me_ref[0] * count

    def search(_, bounds):
        low, high = bounds
        middle = (low + high) // 2
        inside = (low < high) & (ids_ref[jnp.minimum(middle, m - 1)] < start)
        return jnp.where(inside, middle + 1, low), jnp.where(inside, high, jnp.where(low < high, middle, high))

    first, _ = lax.fori_loop(0, m.bit_length(), search, (jnp.int32(0), jnp.int32(m)))
    sub = lax.broadcasted_iota(jnp.int32, (8, B), 0)
    groups = []
    for g in range(cap // 8):
        slots = jnp.zeros((8, B), jnp.int32)
        for i in range(8):
            slots = jnp.where(sub == i, ids_ref[jnp.minimum(first + 8 * g + i, m - 1)] - start, slots)
        groups.append(slots)
    slots = jnp.concatenate(groups, axis=0)
    lane = lax.broadcasted_iota(jnp.int32, (cap, B), 1)
    picks = [(slots == lane + c * B).astype(jnp.float32).astype(jnp.bfloat16) for c in range(count // B)]
    rows_ref[...] = dot(jnp.concatenate(picks, axis=1), points_ref[...]).astype(rows_ref.dtype)
    size = low_ref.shape[1]
    device = lax.broadcasted_iota(jnp.int32, (size, m), 0)
    line = jnp.broadcast_to(line_ref[...], (size, m))
    ones = jnp.ones((8, m), jnp.bfloat16)
    low = dot_nt(ones, (line < device * count).astype(jnp.float32).astype(jnp.bfloat16))
    high = dot_nt(ones, (line < (device + 1) * count).astype(jnp.float32).astype(jnp.bfloat16))
    low_ref[...] = low[0:1].astype(jnp.int32)
    most_ref[...] = jnp.broadcast_to(jnp.max(high - low, axis=1, keepdims=True)[0:1], most_ref.shape).astype(jnp.int32)


def exchange(x, bit):
    dev = lax.axis_size("dev")
    axis, flip = ("dev", bit) if bit < dev else ("grp", bit // dev)
    size = lax.axis_size(axis)
    return lax.ppermute(x, axis, [(k, k ^ flip) for k in range(size)])


def join(parts):
    size = parts[0].shape[0]
    total = size * len(parts)
    lowest = jnp.array(-jnp.inf, parts[0].dtype)
    return functools.reduce(jnp.maximum, [
        lax.pad(part, lowest, ((k * size, total - (k + 1) * size, 0), (0, 0, 0))) for k, part in enumerate(parts)
    ])


def shards(points, ridge, landmark_ids):
    count, width = points.shape
    m = landmark_ids.shape[0]
    devices = lax.axis_size(AXES)
    me = lax.axis_index(AXES)
    mean = m / devices
    cap = min(m, 16 * math.ceil((mean + 5.6 * math.sqrt(mean)) / 16))
    bits = [1 << b for b in range(devices.bit_length() - 1)]
    near = [bit for bit in bits[1:] if bit < lax.axis_size("dev")]
    far = [bit for bit in bits[1:] if bit >= lax.axis_size("dev")]
    order = (*near, *far, bits[0])
    vmem = pl.BlockSpec(memory_space=pltpu.VMEM)
    table = -(-devices // B) * B

    rows, low, most, kept = pl.pallas_call(
        functools.partial(pack, devices),
        grid_spec=pltpu.PrefetchScalarGridSpec(
            num_scalar_prefetch=2, grid=(), in_specs=[vmem, vmem], out_specs=[vmem] * 4,
        ),
        out_shape=(
            jax.ShapeDtypeStruct((cap, width), points.dtype),
            jax.ShapeDtypeStruct((1, table), jnp.int32),
            jax.ShapeDtypeStruct((1, B), jnp.int32),
            pltpu.VMEM((count, width), points.dtype),
        ),
        compiler_params=pltpu.CompilerParams(vmem_limit_bytes=16 << 20),
        name="pack",
    )(me[None], landmark_ids, landmark_ids[None, :], points)
    fits = most[0, 0] <= cap

    groups = [some[at:at + 2] for some in (near, far) for at in range(0, len(some), 2)]
    count_pieces = 2 << len(groups[-1])

    def packed(rows, points, ids):
        for k, pair in enumerate(groups):
            moves = pair if len(pair) == 1 else (pair[0], pair[1], pair[0] | pair[1])
            parts = [rows, *(exchange(rows, move) for move in moves)]
            if k + 1 < len(groups):
                rows = join(parts)
        return *parts, *(exchange(part, bits[0]) for part in parts)

    def summed(rows, points, ids):
        offset = ids - me * count
        inside = (offset >= 0) & (offset < count)
        picked = points[jnp.clip(offset, 0, count - 1)]
        rows = lax.psum(jnp.where(inside[:, None], picked.astype(jnp.float32), 0.0), AXES).astype(points.dtype)
        rows = jnp.pad(rows, ((0, devices * cap - m), (0, 0)))
        return tuple(jnp.split(rows, count_pieces, axis=0))

    pieces = lax.cond(fits, packed, summed, rows, points, landmark_ids)
    info = jnp.stack([fits.astype(jnp.int32), me])

    raw, stat = pl.pallas_call(
        functools.partial(kernel, order),
        grid_spec=pltpu.PrefetchScalarGridSpec(
            num_scalar_prefetch=2,
            grid=(),
            in_specs=[vmem] * (len(pieces) + 2),
            out_specs=[vmem, vmem],
            scratch_shapes=[
                pltpu.VMEM((m, width), jnp.bfloat16),
                pltpu.VMEM((devices * cap, width), jnp.bfloat16),
                pltpu.VMEM((width // B, m + cap, B), jnp.float32),
                pltpu.VMEM((8, m), jnp.float32),
                pltpu.VMEM((m // S, m, S), jnp.float32),
                pltpu.VMEM((3, B, B), jnp.float32),
                pltpu.VMEM((2 * B, B), jnp.float32),
                pltpu.VMEM((4, m, S), jnp.bfloat16),
                pltpu.VMEM((2, m, m), jnp.bfloat16),
                pltpu.VMEM((2, S, S), jnp.bfloat16),
                pltpu.VMEM((4, count, S), jnp.bfloat16),
            ],
        ),
        out_shape=(pltpu.VMEM((m // S, count, S), jnp.float32), jax.ShapeDtypeStruct((2, m), jnp.float32)),
        compiler_params=pltpu.CompilerParams(vmem_limit_bytes=40 << 20),
        name="nystrom",
    )(info, low[0], *pieces, kept, ridge[None, :])

    total = count
    flips = [bit | near[0] if bit in near[1:2] else bit for bit in bits]
    for flip in flips:
        other = exchange(stat, flip)
        delta = other[0] - stat[0]
        stat = jnp.stack([0.5 * (stat[0] + other[0]), stat[1] + other[1] + jnp.square(delta) * (0.5 * total)])
        total *= 2
    gain = 1.0 / jnp.sqrt(stat[1:2] / total + 1e-05)
    steps = 8
    return pl.pallas_call(
        standardize,
        in_specs=[vmem] * 3,
        out_specs=pl.BlockSpec(memory_space=pl.ANY),
        scratch_shapes=[pltpu.VMEM((steps, count // steps, m), jnp.bfloat16), pltpu.SemaphoreType.DMA((steps,))],
        out_shape=jax.ShapeDtypeStruct((count, m), jnp.bfloat16),
        compiler_params=pltpu.CompilerParams(vmem_limit_bytes=16 << 20),
        name="standardize",
    )(raw, stat[0:1], gain)


def solution(mesh):
    placed = (P(AXES, None), P(), P())
    return jax.shard_map(shards, mesh=mesh, in_specs=placed, out_specs=P(AXES, None), check_vma=False)
```

```python
import functools
import math

import jax
import jax.numpy as jnp
from jax import lax
from jax.experimental import pallas as pl
from jax.experimental.pallas import tpu as pltpu
from jax.sharding import PartitionSpec as P

AXES = ("grp", "dev")
B = 128
S = 256
HEAD, FAR = 5, 7
ROWS = 512


def split(x):
    hi = x.astype(jnp.bfloat16)
    return hi, (x - hi.astype(jnp.float32)).astype(jnp.bfloat16)


def dot(left, right, dims=((1,), (0,))):
    return lax.dot_general(left, right, (dims, ((), ())), preferred_element_type=jnp.float32)


def dot_nt(left, right):
    return dot(left, right, ((1,), (1,)))


def dot3(left, right):
    return dot(left[0], right[0]) + dot(left[1], right[0]) + dot(left[0], right[1])


def dot3_narrow(left, right):
    left = jnp.concatenate([left[0], left[1], left[0]], axis=1)
    right = jnp.concatenate([right[0], right[0], right[1]], axis=0)
    return dot(left, right)


def factor_block(d_ref, c_ref, sub, lane):
    n = B // 8
    rows = [d_ref[8 * t:8 * t + 8, :] for t in range(n)]

    def column(t, at):
        return jnp.broadcast_to(rows[t][:, at:at + 1], (8, B))

    def spread(at):
        return jnp.broadcast_to(c_ref[at:at + 1, :], (8, B))

    ahead = [column(0, b) for b in range(8)]
    done = []
    for k in range(n):
        stop = FAR if k < HEAD else n
        first = 8 * k
        base = (k % 2) * 128
        follow = k + 1 < n
        for b in range(8):
            c_ref[base + 8 * b:base + 8 * b + 8, :] = ahead[b]
        s = {(a, b): spread(base + 8 * b + a) for b in range(8) for a in range(b + 1)}
        if follow:
            z = [column(k + 1, first + j) for j in range(8)]
            ahead = [column(k + 1, first + 8 + b) for b in range(8)]
            acc = rows[k + 1]
        below = {t: [column(t, first + j) for j in range(7, -1, -1)][::-1] for t in range(k + 2, stop)}
        pivot = (lane >= first) & (lane < first + 8)
        start = jnp.where(pivot, (lane - first == sub).astype(jnp.float32), rows[k])
        y = [jnp.broadcast_to(start[i:i + 1, :], (8, B)) for i in range(8)]
        if follow:
            acc = jnp.where(pivot, 0.0, acc)
        inv = []
        for j in range(8):
            r = lax.rsqrt(s[(j, j)])
            inv.append(r)
            for b in range(j + 1, 8):
                s[(j, b)] = s[(j, b)] * r
            y[j] = y[j] * r
            if follow:
                z[j] = z[j] * r
                acc = acc - z[j] * y[j]
                at = base + 64 + 8 * j
                c_ref[at:at + 8, :] = z[j]
                for b in range(8):
                    ahead[b] = ahead[b] - z[j] * spread(at + b)
            for b in range(j + 1, 8):
                for a in range(j + 1, b + 1):
                    s[(a, b)] = s[(a, b)] - s[(j, a)] * s[(j, b)]
            for b in range(j + 1, 8):
                y[b] = y[b] - s[(j, b)] * y[j]
                if follow:
                    z[b] = z[b] - s[(j, b)] * z[j]
        w = y[7]
        for i in range(7):
            w = jnp.where(sub == i, y[i], w)
        d_ref[first:first + 8, :] = jnp.where(lane < first + 8, w, 0.0)
        done.append(w)
        if follow:
            rows[k + 1] = acc
        if k + 2 < n:
            q = [None] * 8
            for j in range(7, -1, -1):
                v = y[j]
                for i in range(7, j, -1):
                    v = v - s[(j, i)] * q[i]
                q[j] = v * inv[j]
            for t in range(k + 2, stop):
                v = jnp.where(pivot, 0.0, rows[t])
                for j in range(7, -1, -1):
                    v = v - below[t][j] * q[j]
                rows[t] = v
        if k == HEAD - 1:
            left = split(jnp.concatenate(done, axis=0))
            kept = [jnp.where((lane < 8 * i + 8) | (lane >= 8 * HEAD), u, 0.0) for i, u in enumerate(done)]
            right = split(jnp.concatenate(kept, axis=0))
            left = jnp.concatenate([left[0], left[1], left[0]], axis=0)
            right = jnp.concatenate([right[0], right[0], right[1]], axis=0)
            part = dot(left, right, ((0,), (0,)))
            for t in range(FAR, n):
                rows[t] = jnp.where(lane < 8 * HEAD, 0.0, rows[t]) - part[8 * t:8 * t + 8]
        yield k


def square_sums(x):
    hi, lo = split(jnp.square(x.astype(jnp.float32)))
    both = jnp.concatenate([hi, lo], axis=1)
    return dot_nt(jnp.ones((8, both.shape[1]), jnp.bfloat16), both), dot_nt(both, jnp.ones((B, both.shape[1]), jnp.bfloat16))


def wide(x):
    return jnp.concatenate([x] * (S // B), axis=1)


def kernel(order, info_ref, low_ref, *refs):
    (*piece_refs, points_ref, ridge_ref, x_ref, stat_ref, marks_ref, rows_ref, packed_ref, along_ref, a_ref, d_ref,
     c_ref, l_ref, lt_ref, wt_ref, r_ref, norm_ref) = refs
    m, width = marks_ref.shape
    count = points_ref.shape[0]
    scale = 1.0 / (2.0 * width)
    cap = packed_ref.shape[1] - m
    stages = m // S
    half = count // 2
    sub = lax.broadcasted_iota(jnp.int32, (8, B), 0)
    lane = lax.broadcasted_iota(jnp.int32, (8, B), 1)

    size = piece_refs[0].shape[0]
    for k, piece_ref in enumerate(piece_refs):
        rows_ref[k * size:(k + 1) * size, :] = piece_ref[...]

    def place(d, carry):
        packed = info_ref[0] != 0
        far = d ^ info_ref[1]
        block = 0
        for k, bit in enumerate(order):
            block = block + jnp.where((far & bit) != 0, 1 << k, 0)
        plain = d % (m // cap)
        source = jnp.where(packed, block, plain) * cap
        target = jnp.where(packed, low_ref[d], plain * cap)
        rows = rows_ref[pl.ds(pl.multiple_of(source, cap), cap), :].astype(jnp.float32)
        for c in range(width // B):
            packed_ref[c, pl.ds(target, cap), :] = rows[:, c * B:(c + 1) * B]
        return carry

    lax.fori_loop(0, 1 << len(order), place, 0)
    marks_ref[...] = jnp.concatenate([packed_ref[c, :m] for c in range(width // B)], axis=1).astype(jnp.bfloat16)
    marks = marks_ref[...]
    along, down = square_sums(marks)
    along_ref[...] = along
    down = wide(down)
    stat_ref[...] = jnp.zeros_like(stat_ref)
    row = lax.broadcasted_iota(jnp.int32, (S, S), 0)
    col = lax.broadcasted_iota(jnp.int32, (S, S), 1)
    for j in range(stages):
        here = slice(j * S, (j + 1) * S)
        inner = dot_nt(marks[j * S:], marks[here])
        a_ref[j, j * S:, :] = jnp.exp(-(down[j * S:] + along[0:1, here] - 2.0 * inner) * scale)
        a_ref[j, here, :] += jnp.where(row == col, ridge_ref[0:1, here], 0.0)
    d_ref[0] = a_ref[0, :B, :B]

    def cross_piece(j, at):
        here = slice(j * S, (j + 1) * S)
        rows = pl.ds(at, ROWS)
        points = points_ref[rows, :]
        if j == 0:
            norm_ref[rows, :] = square_sums(points)[1]
        inner = dot_nt(points, marks_ref[here, :])
        x_ref[j, rows, :] = jnp.exp(-(wide(norm_ref[rows, :]) + along_ref[0:1, here] - 2.0 * inner) * scale)

    def raw_piece(p, at):
        here = slice(p * S, (p + 1) * S)
        rows = pl.ds(at, ROWS)
        raw = dot3(split(x_ref[p, rows, :]), (wt_ref[0], wt_ref[1]))
        x_ref[p, rows, :] = raw
        keep = 2 * (p % 2)
        r_ref[keep, rows, :], r_ref[keep + 1, rows, :] = split(raw)
        mean = jnp.mean(raw, axis=0, keepdims=True)
        spread = jnp.sum(jnp.square(raw - mean), axis=0, keepdims=True)
        before = jnp.asarray(at).astype(jnp.float32)
        share = ROWS / (before + ROWS)
        delta = mean - stat_ref[0:1, here]
        stat_ref[1:2, here] += spread + jnp.square(delta) * (before * share)
        stat_ref[0:1, here] += delta * share

    def update_piece(p, j, at):
        rows = pl.ds(at, ROWS)
        right = [lt_ref[h, p * S:(p + 1) * S, j * S:(j + 1) * S] for h in range(2)]
        keep = 2 * (p % 2)
        x_ref[j, rows, :] -= dot3((r_ref[keep, rows, :], r_ref[keep + 1, rows, :]), right)

    def core_piece(p, j, odd):
        size = (m - j * S) // 2
        rows = pl.ds(pl.multiple_of(j * S + odd * size, B), size)
        right = [lt_ref[h, p * S:(p + 1) * S, j * S:(j + 1) * S] for h in range(2)]
        keep = 2 * (p % 2)
        a_ref[j, rows, :] -= dot3((l_ref[keep, rows, :], l_ref[keep + 1, rows, :]), right)

    def finish(p, odd):
        top = p * S + (odd + 1) * B
        here = slice(odd * B, (odd + 1) * B)
        at = slice(p * S + odd * B, p * S + (odd + 1) * B)
        keep = 2 * (p % 2)
        wt = jnp.transpose(d_ref[0])
        if top < m:
            block = dot3_narrow(split(a_ref[p, top:, here]), split(wt))
            left = split(block)
            right = split(jnp.transpose(block))
            for h in range(2):
                l_ref[keep + h, top:, here] = left[h]
                lt_ref[h, at, top:] = right[h]
        if odd == 0:
            a_ref[p, top:, B:] -= dot3_narrow(left, [r[:, :B] for r in right])
            d_ref[1] = wt
            d_ref[2] = jnp.transpose(block[:B])
            d_ref[0] = a_ref[p, top:top + B, B:]
        else:
            first = d_ref[1]
            inner = dot3_narrow(split(d_ref[2]), split(wt))
            corner = -dot3_narrow(split(first), split(inner))
            upper = jnp.concatenate([first, corner], axis=1)
            lower = jnp.concatenate([jnp.zeros_like(wt), wt], axis=1)
            wt_ref[0], wt_ref[1] = split(jnp.concatenate([upper, lower], axis=0))
            if top < m:
                right = [lt_ref[h, p * S:top, top:top + S] for h in range(2)]
                a_ref[p + 1, top:, :] -= dot3((l_ref[keep, top:, :], l_ref[keep + 1, top:, :]), right)
                d_ref[0] = a_ref[p + 1, top:top + B, :B]

    def turn(q, j):
        return q + 2 if q and j > q + 1 else min(max(j - 1, q + 1), q + 2)

    for p in range(stages):
        def stage(odd, carry, p=p):
            pieces = []
            for j in range(p + 1, stages):
                if p:
                    pieces.append(functools.partial(core_piece, p - 1, j, odd))
            for block in range(half // ROWS):
                at = pl.multiple_of(odd * half + block * ROWS, ROWS)
                if p:
                    pieces.append(functools.partial(raw_piece, p - 1, at))
                for j in range(stages):
                    if p == min(max(j - 1, 0), 2):
                        pieces.append(functools.partial(cross_piece, j, at))
                    pieces += [functools.partial(update_piece, q, j, at) for q in range(j) if p == turn(q, j)]
            done = 0
            for k in factor_block(d_ref.at[0], c_ref, sub, lane):
                until = -(-len(pieces) * (k + 1) // 14)
                for piece in pieces[done:until]:
                    piece()
                done = max(done, until)
            for o in range(2):
                pl.when(odd == o)(functools.partial(finish, p, o))
            return carry

        lax.fori_loop(0, 2, stage, 0)

    def last(odd, carry):
        for block in range(half // ROWS):
            raw_piece(stages - 1, pl.multiple_of(odd * half + block * ROWS, ROWS))
        return carry

    lax.fori_loop(0, 2, last, 0)


def standardize(x_ref, shift_ref, gain_ref, out_hbm, out_ref, sems):
    steps, size, _ = out_ref.shape

    def copy(k):
        return pltpu.make_async_copy(out_ref.at[k], out_hbm.at[k * size:(k + 1) * size, :], sems.at[k])

    for k in range(steps):
        for p in range(x_ref.shape[0]):
            here = slice(p * S, (p + 1) * S)
            x = x_ref[p, k * size:(k + 1) * size, :]
            out_ref[k, :, here] = ((x - shift_ref[:, here]) * gain_ref[:, here]).astype(out_ref.dtype)
        copy(k).start()
    for k in range(steps):
        copy(k).wait()


def pack(devices, me_ref, ids_ref, line_ref, points_ref, rows_ref, low_ref, most_ref, kept_ref):
    cap = rows_ref.shape[0]
    count = points_ref.shape[0]
    m = ids_ref.shape[0]
    kept_ref[...] = points_ref[...]
    start = me_ref[0] * count

    def search(_, bounds):
        low, high = bounds
        middle = (low + high) // 2
        inside = (low < high) & (ids_ref[jnp.minimum(middle, m - 1)] < start)
        return jnp.where(inside, middle + 1, low), jnp.where(inside, high, jnp.where(low < high, middle, high))

    first, _ = lax.fori_loop(0, m.bit_length(), search, (jnp.int32(0), jnp.int32(m)))
    sub = lax.broadcasted_iota(jnp.int32, (8, B), 0)
    groups = []
    for g in range(cap // 8):
        slots = jnp.zeros((8, B), jnp.int32)
        for i in range(8):
            slots = jnp.where(sub == i, ids_ref[jnp.minimum(first + 8 * g + i, m - 1)] - start, slots)
        groups.append(slots)
    slots = jnp.concatenate(groups, axis=0)
    lane = lax.broadcasted_iota(jnp.int32, (cap, B), 1)
    picks = [(slots == lane + c * B).astype(jnp.float32).astype(jnp.bfloat16) for c in range(count // B)]
    rows_ref[...] = dot(jnp.concatenate(picks, axis=1), points_ref[...]).astype(rows_ref.dtype)
    size = low_ref.shape[1]
    device = lax.broadcasted_iota(jnp.int32, (size, m), 0)
    line = jnp.broadcast_to(line_ref[...], (size, m))
    ones = jnp.ones((8, m), jnp.bfloat16)
    low = dot_nt(ones, (line < device * count).astype(jnp.float32).astype(jnp.bfloat16))
    high = dot_nt(ones, (line < (device + 1) * count).astype(jnp.float32).astype(jnp.bfloat16))
    low_ref[...] = low[0:1].astype(jnp.int32)
    most_ref[...] = jnp.broadcast_to(jnp.max(high - low, axis=1, keepdims=True)[0:1], most_ref.shape).astype(jnp.int32)


def exchange(x, bit):
    dev = lax.axis_size("dev")
    axis, flip = ("dev", bit) if bit < dev else ("grp", bit // dev)
    size = lax.axis_size(axis)
    return lax.ppermute(x, axis, [(k, k ^ flip) for k in range(size)])


def join(parts):
    size = parts[0].shape[0]
    total = size * len(parts)
    lowest = jnp.array(-jnp.inf, parts[0].dtype)
    return functools.reduce(jnp.maximum, [
        lax.pad(part, lowest, ((k * size, total - (k + 1) * size, 0), (0, 0, 0))) for k, part in enumerate(parts)
    ])


def shards(points, ridge, landmark_ids):
    count, width = points.shape
    m = landmark_ids.shape[0]
    devices = lax.axis_size(AXES)
    me = lax.axis_index(AXES)
    mean = m / devices
    cap = min(m, 16 * math.ceil((mean + 5.6 * math.sqrt(mean)) / 16))
    bits = [1 << b for b in range(devices.bit_length() - 1)]
    near = [bit for bit in bits[1:] if bit < lax.axis_size("dev")]
    far = [bit for bit in bits[1:] if bit >= lax.axis_size("dev")]
    order = (*near, *far, bits[0])
    vmem = pl.BlockSpec(memory_space=pltpu.VMEM)
    table = -(-devices // B) * B

    rows, low, most, kept = pl.pallas_call(
        functools.partial(pack, devices),
        grid_spec=pltpu.PrefetchScalarGridSpec(
            num_scalar_prefetch=2, grid=(), in_specs=[vmem, vmem], out_specs=[vmem] * 4,
        ),
        out_shape=(
            jax.ShapeDtypeStruct((cap, width), points.dtype),
            jax.ShapeDtypeStruct((1, table), jnp.int32),
            jax.ShapeDtypeStruct((1, B), jnp.int32),
            pltpu.VMEM((count, width), points.dtype),
        ),
        compiler_params=pltpu.CompilerParams(vmem_limit_bytes=16 << 20),
        name="pack",
    )(me[None], landmark_ids, landmark_ids[None, :], points)
    fits = most[0, 0] <= cap

    groups = [some[at:at + 2] for some in (near, far) for at in range(0, len(some), 2)]
    count_pieces = 2 << len(groups[-1])

    def packed(rows, points, ids):
        for k, pair in enumerate(groups):
            moves = pair if len(pair) == 1 else (pair[0], pair[1], pair[0] | pair[1])
            parts = [rows, *(exchange(rows, move) for move in moves)]
            if k + 1 < len(groups):
                rows = join(parts)
        return *parts, *(exchange(part, bits[0]) for part in parts)

    def summed(rows, points, ids):
        offset = ids - me * count
        inside = (offset >= 0) & (offset < count)
        picked = points[jnp.clip(offset, 0, count - 1)]
        rows = lax.psum(jnp.where(inside[:, None], picked.astype(jnp.float32), 0.0), AXES).astype(points.dtype)
        rows = jnp.pad(rows, ((0, devices * cap - m), (0, 0)))
        return tuple(jnp.split(rows, count_pieces, axis=0))

    pieces = lax.cond(fits, packed, summed, rows, points, landmark_ids)
    info = jnp.stack([fits.astype(jnp.int32), me])

    raw, stat = pl.pallas_call(
        functools.partial(kernel, order),
        grid_spec=pltpu.PrefetchScalarGridSpec(
            num_scalar_prefetch=2,
            grid=(),
            in_specs=[vmem] * (len(pieces) + 2),
            out_specs=[vmem, vmem],
            scratch_shapes=[
                pltpu.VMEM((m, width), jnp.bfloat16),
                pltpu.VMEM((devices * cap, width), jnp.bfloat16),
                pltpu.VMEM((width // B, m + cap, B), jnp.float32),
                pltpu.VMEM((8, m), jnp.float32),
                pltpu.VMEM((m // S, m, S), jnp.float32),
                pltpu.VMEM((3, B, B), jnp.float32),
                pltpu.VMEM((2 * B, B), jnp.float32),
                pltpu.VMEM((4, m, S), jnp.bfloat16),
                pltpu.VMEM((2, m, m), jnp.bfloat16),
                pltpu.VMEM((2, S, S), jnp.bfloat16),
                pltpu.VMEM((4, count, S), jnp.bfloat16),
                pltpu.VMEM((count, B), jnp.float32),
            ],
        ),
        out_shape=(pltpu.VMEM((m // S, count, S), jnp.float32), jax.ShapeDtypeStruct((2, m), jnp.float32)),
        compiler_params=pltpu.CompilerParams(vmem_limit_bytes=40 << 20),
        name="nystrom",
    )(info, low[0], *pieces, kept, ridge[None, :])

    total = count
    flips = [bit | near[0] if bit in near[1:2] else bit for bit in bits]
    for flip in flips:
        other = exchange(stat, flip)
        delta = other[0] - stat[0]
        stat = jnp.stack([0.5 * (stat[0] + other[0]), stat[1] + other[1] + jnp.square(delta) * (0.5 * total)])
        total *= 2
    gain = 1.0 / jnp.sqrt(stat[1:2] / total + 1e-05)
    steps = 8
    return pl.pallas_call(
        standardize,
        in_specs=[vmem] * 3,
        out_specs=pl.BlockSpec(memory_space=pl.ANY),
        scratch_shapes=[pltpu.VMEM((steps, count // steps, m), jnp.bfloat16), pltpu.SemaphoreType.DMA((steps,))],
        out_shape=jax.ShapeDtypeStruct((count, m), jnp.bfloat16),
        compiler_params=pltpu.CompilerParams(vmem_limit_bytes=16 << 20),
        name="standardize",
    )(raw, stat[0:1], gain)


def solution(mesh):
    placed = (P(AXES, None), P(), P())
    return jax.shard_map(shards, mesh=mesh, in_specs=placed, out_specs=P(AXES, None), check_vma=False)
```

```python
import functools
import math

import jax
import jax.numpy as jnp
from jax import lax
from jax.experimental import pallas as pl
from jax.experimental.pallas import tpu as pltpu
from jax.sharding import PartitionSpec as P

AXES = ("grp", "dev")
B = 128
S = 256
HEAD, FAR = 5, 7
ROWS = 512


def split(x):
    hi = x.astype(jnp.bfloat16)
    return hi, (x - hi.astype(jnp.float32)).astype(jnp.bfloat16)


def dot(left, right, dims=((1,), (0,))):
    return lax.dot_general(left, right, (dims, ((), ())), preferred_element_type=jnp.float32)


def dot_nt(left, right):
    return dot(left, right, ((1,), (1,)))


def dot3(left, right):
    return dot(left[0], right[0]) + dot(left[1], right[0]) + dot(left[0], right[1])


def dot3_narrow(left, right):
    left = jnp.concatenate([left[0], left[1], left[0]], axis=1)
    right = jnp.concatenate([right[0], right[0], right[1]], axis=0)
    return dot(left, right)


def factor_block(d_ref, c_ref, sub, lane):
    n = B // 8
    rows = [d_ref[8 * t:8 * t + 8, :] for t in range(n)]

    def column(t, at):
        return jnp.broadcast_to(rows[t][:, at:at + 1], (8, B))

    def spread(at):
        return jnp.broadcast_to(c_ref[at:at + 1, :], (8, B))

    ahead = [column(0, b) for b in range(8)]
    done = []
    for k in range(n):
        stop = FAR if k < HEAD else n
        first = 8 * k
        base = (k % 2) * 128
        follow = k + 1 < n
        for b in range(8):
            c_ref[base + 8 * b:base + 8 * b + 8, :] = ahead[b]
        s = {(a, b): spread(base + 8 * b + a) for b in range(8) for a in range(b + 1)}
        if follow:
            z = [column(k + 1, first + j) for j in range(8)]
            ahead = [column(k + 1, first + 8 + b) for b in range(8)]
            acc = rows[k + 1]
        below = {t: [column(t, first + j) for j in range(7, -1, -1)][::-1] for t in range(k + 2, stop)}
        pivot = (lane >= first) & (lane < first + 8)
        start = jnp.where(pivot, (lane - first == sub).astype(jnp.float32), rows[k])
        y = [jnp.broadcast_to(start[i:i + 1, :], (8, B)) for i in range(8)]
        if follow:
            acc = jnp.where(pivot, 0.0, acc)
        inv = []
        for j in range(8):
            r = lax.rsqrt(s[(j, j)])
            inv.append(r)
            for b in range(j + 1, 8):
                s[(j, b)] = s[(j, b)] * r
            y[j] = y[j] * r
            if follow:
                z[j] = z[j] * r
                acc = acc - z[j] * y[j]
                at = base + 64 + 8 * j
                c_ref[at:at + 8, :] = z[j]
                for b in range(8):
                    ahead[b] = ahead[b] - z[j] * spread(at + b)
            for b in range(j + 1, 8):
                for a in range(j + 1, b + 1):
                    s[(a, b)] = s[(a, b)] - s[(j, a)] * s[(j, b)]
            for b in range(j + 1, 8):
                y[b] = y[b] - s[(j, b)] * y[j]
                if follow:
                    z[b] = z[b] - s[(j, b)] * z[j]
        w = y[7]
        for i in range(7):
            w = jnp.where(sub == i, y[i], w)
        d_ref[first:first + 8, :] = jnp.where(lane < first + 8, w, 0.0)
        done.append(w)
        if follow:
            rows[k + 1] = acc
        if k + 2 < n:
            q = [None] * 8
            for j in range(7, -1, -1):
                v = y[j]
                for i in range(7, j, -1):
                    v = v - s[(j, i)] * q[i]
                q[j] = v * inv[j]
            for t in range(k + 2, stop):
                v = jnp.where(pivot, 0.0, rows[t])
                for j in range(7, -1, -1):
                    v = v - below[t][j] * q[j]
                rows[t] = v
        if k == HEAD - 1:
            left = split(jnp.concatenate(done, axis=0))
            kept = [jnp.where((lane < 8 * i + 8) | (lane >= 8 * HEAD), u, 0.0) for i, u in enumerate(done)]
            right = split(jnp.concatenate(kept, axis=0))
            left = jnp.concatenate([left[0], left[1], left[0]], axis=0)
            right = jnp.concatenate([right[0], right[0], right[1]], axis=0)
            part = dot(left, right, ((0,), (0,)))
            for t in range(FAR, n):
                rows[t] = jnp.where(lane < 8 * HEAD, 0.0, rows[t]) - part[8 * t:8 * t + 8]
        yield k


def square_sums(x):
    hi, lo = split(jnp.square(x.astype(jnp.float32)))
    both = jnp.concatenate([hi, lo], axis=1)
    return dot_nt(jnp.ones((8, both.shape[1]), jnp.bfloat16), both), dot_nt(both, jnp.ones((B, both.shape[1]), jnp.bfloat16))


def wide(x):
    return jnp.concatenate([x] * (S // B), axis=1)


def kernel(order, info_ref, low_ref, *refs):
    (*piece_refs, points_ref, ridge_ref, x_ref, stat_ref, marks_ref, rows_ref, packed_ref, along_ref, a_ref, d_ref,
     c_ref, l_ref, lt_ref, wt_ref, r_ref, norm_ref) = refs
    m, width = marks_ref.shape
    count = points_ref.shape[0]
    scale = 1.0 / (2.0 * width)
    cap = packed_ref.shape[1] - m
    stages = m // S
    half = count // 2
    sub = lax.broadcasted_iota(jnp.int32, (8, B), 0)
    lane = lax.broadcasted_iota(jnp.int32, (8, B), 1)

    size = piece_refs[0].shape[0]
    for k, piece_ref in enumerate(piece_refs):
        rows_ref[k * size:(k + 1) * size, :] = piece_ref[...]

    def place(d, carry):
        packed = info_ref[0] != 0
        far = d ^ info_ref[1]
        block = 0
        for k, bit in enumerate(order):
            block = block + jnp.where((far & bit) != 0, 1 << k, 0)
        plain = d % (m // cap)
        source = jnp.where(packed, block, plain) * cap
        target = jnp.where(packed, low_ref[d], plain * cap)
        rows = rows_ref[pl.ds(pl.multiple_of(source, cap), cap), :].astype(jnp.float32)
        for c in range(width // B):
            packed_ref[c, pl.ds(target, cap), :] = rows[:, c * B:(c + 1) * B]
        return carry

    lax.fori_loop(0, 1 << len(order), place, 0)
    marks_ref[...] = jnp.concatenate([packed_ref[c, :m] for c in range(width // B)], axis=1).astype(jnp.bfloat16)
    marks = marks_ref[...]
    along, down = square_sums(marks)
    along_ref[...] = along
    down = wide(down)
    stat_ref[...] = jnp.zeros_like(stat_ref)
    row = lax.broadcasted_iota(jnp.int32, (S, S), 0)
    col = lax.broadcasted_iota(jnp.int32, (S, S), 1)
    for j in range(stages):
        here = slice(j * S, (j + 1) * S)
        inner = dot_nt(marks[j * S:], marks[here])
        a_ref[j, j * S:, :] = jnp.exp(-(down[j * S:] + along[0:1, here] - 2.0 * inner) * scale)
        a_ref[j, here, :] += jnp.where(row == col, ridge_ref[0:1, here], 0.0)
    d_ref[0] = a_ref[0, :B, :B]

    def cross_piece(j, at):
        here = slice(j * S, (j + 1) * S)
        rows = pl.ds(at, ROWS)
        points = points_ref[rows, :]
        if j == 0:
            norm_ref[rows, :] = square_sums(points)[1]
        inner = dot_nt(points, marks_ref[here, :])
        x_ref[j, rows, :] = jnp.exp(-(wide(norm_ref[rows, :]) + along_ref[0:1, here] - 2.0 * inner) * scale)

    def raw_piece(p, at):
        here = slice(p * S, (p + 1) * S)
        rows = pl.ds(at, ROWS)
        raw = dot3(split(x_ref[p, rows, :]), (wt_ref[0], wt_ref[1]))
        x_ref[p, rows, :] = raw
        keep = 2 * (p % 2)
        r_ref[keep, rows, :], r_ref[keep + 1, rows, :] = split(raw)
        mean = jnp.mean(raw, axis=0, keepdims=True)
        spread = jnp.sum(jnp.square(raw - mean), axis=0, keepdims=True)
        before = jnp.asarray(at).astype(jnp.float32)
        share = ROWS / (before + ROWS)
        delta = mean - stat_ref[0:1, here]
        stat_ref[1:2, here] += spread + jnp.square(delta) * (before * share)
        stat_ref[0:1, here] += delta * share

    def update_piece(p, j, at):
        rows = pl.ds(at, ROWS)
        right = [lt_ref[h, p * S:(p + 1) * S, j * S:(j + 1) * S] for h in range(2)]
        keep = 2 * (p % 2)
        x_ref[j, rows, :] -= dot3((r_ref[keep, rows, :], r_ref[keep + 1, rows, :]), right)

    def core_piece(p, j, odd):
        size = (m - j * S) // 2
        rows = pl.ds(pl.multiple_of(j * S + odd * size, B), size)
        right = [lt_ref[h, p * S:(p + 1) * S, j * S:(j + 1) * S] for h in range(2)]
        keep = 2 * (p % 2)
        a_ref[j, rows, :] -= dot3((l_ref[keep, rows, :], l_ref[keep + 1, rows, :]), right)

    def finish(p, odd):
        top = p * S + (odd + 1) * B
        here = slice(odd * B, (odd + 1) * B)
        at = slice(p * S + odd * B, p * S + (odd + 1) * B)
        keep = 2 * (p % 2)
        wt = jnp.transpose(d_ref[0])
        if top < m:
            block = dot3_narrow(split(a_ref[p, top:, here]), split(wt))
            left = split(block)
            right = split(jnp.transpose(block))
            for h in range(2):
                l_ref[keep + h, top:, here] = left[h]
                lt_ref[h, at, top:] = right[h]
        if odd == 0:
            a_ref[p, top:, B:] -= dot3_narrow(left, [r[:, :B] for r in right])
            d_ref[1] = wt
            d_ref[2] = jnp.transpose(block[:B])
            d_ref[0] = a_ref[p, top:top + B, B:]
        else:
            first = d_ref[1]
            inner = dot3_narrow(split(d_ref[2]), split(wt))
            corner = -dot3_narrow(split(first), split(inner))
            upper = jnp.concatenate([first, corner], axis=1)
            lower = jnp.concatenate([jnp.zeros_like(wt), wt], axis=1)
            wt_ref[0], wt_ref[1] = split(jnp.concatenate([upper, lower], axis=0))
            if top < m:
                right = [lt_ref[h, p * S:top, top:top + S] for h in range(2)]
                a_ref[p + 1, top:, :] -= dot3((l_ref[keep, top:, :], l_ref[keep + 1, top:, :]), right)
                d_ref[0] = a_ref[p + 1, top:top + B, :B]

    def turn(q, j):
        return q + 2 if q and j > q + 1 else min(max(j - 1, q + 1), q + 2)

    for p in range(stages):
        def stage(odd, carry, p=p):
            pieces = []
            for j in range(p + 1, stages):
                if p:
                    pieces.append(functools.partial(core_piece, p - 1, j, odd))
            for block in range(half // ROWS):
                at = pl.multiple_of(odd * half + block * ROWS, ROWS)
                if p:
                    pieces.append(functools.partial(raw_piece, p - 1, at))
                for j in range(stages):
                    if p == min(max(j - 1, 0), 2):
                        pieces.append(functools.partial(cross_piece, j, at))
                    pieces += [functools.partial(update_piece, q, j, at) for q in range(j) if p == turn(q, j)]
            done = 0
            for k in factor_block(d_ref.at[0], c_ref, sub, lane):
                until = -(-len(pieces) * (k + 1) // 14)
                for piece in pieces[done:until]:
                    piece()
                done = max(done, until)
            for o in range(2):
                pl.when(odd == o)(functools.partial(finish, p, o))
            return carry

        lax.fori_loop(0, 2, stage, 0)

    def last(odd, carry):
        for block in range(half // ROWS):
            raw_piece(stages - 1, pl.multiple_of(odd * half + block * ROWS, ROWS))
        return carry

    lax.fori_loop(0, 2, last, 0)


def standardize(x_ref, shift_ref, gain_ref, out_hbm, out_ref, sems):
    steps, size, _ = out_ref.shape

    def copy(k):
        return pltpu.make_async_copy(out_ref.at[k], out_hbm.at[k * size:(k + 1) * size, :], sems.at[k])

    for k in range(steps):
        for p in range(x_ref.shape[0]):
            here = slice(p * S, (p + 1) * S)
            x = x_ref[p, k * size:(k + 1) * size, :]
            out_ref[k, :, here] = ((x - shift_ref[:, here]) * gain_ref[:, here]).astype(out_ref.dtype)
        copy(k).start()
    for k in range(steps):
        copy(k).wait()


def pack(devices, me_ref, ids_ref, line_ref, points_ref, rows_ref, low_ref, most_ref, kept_ref):
    cap = rows_ref.shape[0]
    count = points_ref.shape[0]
    m = ids_ref.shape[0]
    kept_ref[...] = points_ref[...]
    start = me_ref[0] * count

    def search(_, bounds):
        low, high = bounds
        middle = (low + high) // 2
        inside = (low < high) & (ids_ref[jnp.minimum(middle, m - 1)] < start)
        return jnp.where(inside, middle + 1, low), jnp.where(inside, high, jnp.where(low < high, middle, high))

    first, _ = lax.fori_loop(0, m.bit_length(), search, (jnp.int32(0), jnp.int32(m)))
    sub = lax.broadcasted_iota(jnp.int32, (8, B), 0)
    groups = []
    for g in range(cap // 8):
        slots = jnp.zeros((8, B), jnp.int32)
        for i in range(8):
            slots = jnp.where(sub == i, ids_ref[jnp.minimum(first + 8 * g + i, m - 1)] - start, slots)
        groups.append(slots)
    slots = jnp.concatenate(groups, axis=0)
    lane = lax.broadcasted_iota(jnp.int32, (cap, B), 1)
    picks = [(slots == lane + c * B).astype(jnp.float32).astype(jnp.bfloat16) for c in range(count // B)]
    rows_ref[...] = dot(jnp.concatenate(picks, axis=1), points_ref[...]).astype(rows_ref.dtype)
    size = low_ref.shape[1]
    device = lax.broadcasted_iota(jnp.int32, (size, m), 0)
    line = jnp.broadcast_to(line_ref[...], (size, m))
    ones = jnp.ones((8, m), jnp.bfloat16)
    low = dot_nt(ones, (line < device * count).astype(jnp.float32).astype(jnp.bfloat16))
    high = dot_nt(ones, (line < (device + 1) * count).astype(jnp.float32).astype(jnp.bfloat16))
    low_ref[...] = low[0:1].astype(jnp.int32)
    most_ref[...] = jnp.broadcast_to(jnp.max(high - low, axis=1, keepdims=True)[0:1], most_ref.shape).astype(jnp.int32)


def exchange(x, bit):
    dev = lax.axis_size("dev")
    axis, flip = ("dev", bit) if bit < dev else ("grp", bit // dev)
    size = lax.axis_size(axis)
    return lax.ppermute(x, axis, [(k, k ^ flip) for k in range(size)])


def join(parts):
    size = parts[0].shape[0]
    total = size * len(parts)
    lowest = jnp.array(-jnp.inf, parts[0].dtype)
    return functools.reduce(jnp.maximum, [
        lax.pad(part, lowest, ((k * size, total - (k + 1) * size, 0), (0, 0, 0))) for k, part in enumerate(parts)
    ])


def shards(points, ridge, landmark_ids):
    count, width = points.shape
    m = landmark_ids.shape[0]
    devices = lax.axis_size(AXES)
    me = lax.axis_index(AXES)
    mean = m / devices
    cap = min(m, 16 * math.ceil((mean + 5.6 * math.sqrt(mean)) / 16))
    bits = [1 << b for b in range(devices.bit_length() - 1)]
    near = [bit for bit in bits[1:] if bit < lax.axis_size("dev")]
    far = [bit for bit in bits[1:] if bit >= lax.axis_size("dev")]
    order = (*near, *far, bits[0])
    vmem = pl.BlockSpec(memory_space=pltpu.VMEM)
    table = -(-devices // B) * B

    rows, low, most, kept = pl.pallas_call(
        functools.partial(pack, devices),
        grid_spec=pltpu.PrefetchScalarGridSpec(
            num_scalar_prefetch=2, grid=(), in_specs=[vmem, vmem], out_specs=[vmem] * 4,
        ),
        out_shape=(
            jax.ShapeDtypeStruct((cap, width), points.dtype),
            jax.ShapeDtypeStruct((1, table), jnp.int32),
            jax.ShapeDtypeStruct((1, B), jnp.int32),
            pltpu.VMEM((count, width), points.dtype),
        ),
        compiler_params=pltpu.CompilerParams(vmem_limit_bytes=16 << 20),
        name="pack",
    )(me[None], landmark_ids, landmark_ids[None, :], points)
    fits = most[0, 0] <= cap

    groups = [some[at:at + 2] for some in (near, far) for at in range(0, len(some), 2)]
    count_pieces = 2 << len(groups[-1])

    def packed(rows, points, ids):
        for k, pair in enumerate(groups):
            moves = pair if len(pair) == 1 else (pair[0], pair[1], pair[0] | pair[1])
            parts = [rows, *(exchange(rows, move) for move in moves)]
            if k + 1 < len(groups):
                rows = join(parts)
        return *parts, *(exchange(part, bits[0]) for part in parts)

    def summed(rows, points, ids):
        offset = ids - me * count
        inside = (offset >= 0) & (offset < count)
        picked = points[jnp.clip(offset, 0, count - 1)]
        rows = lax.psum(jnp.where(inside[:, None], picked.astype(jnp.float32), 0.0), AXES).astype(points.dtype)
        rows = jnp.pad(rows, ((0, devices * cap - m), (0, 0)))
        return tuple(jnp.split(rows, count_pieces, axis=0))

    pieces = lax.cond(fits, packed, summed, rows, points, landmark_ids)
    info = jnp.stack([fits.astype(jnp.int32), me])

    raw, stat = pl.pallas_call(
        functools.partial(kernel, order),
        grid_spec=pltpu.PrefetchScalarGridSpec(
            num_scalar_prefetch=2,
            grid=(),
            in_specs=[vmem] * (len(pieces) + 2),
            out_specs=[vmem, vmem],
            scratch_shapes=[
                pltpu.VMEM((m, width), jnp.bfloat16),
                pltpu.VMEM((devices * cap, width), jnp.bfloat16),
                pltpu.VMEM((width // B, m + cap, B), jnp.float32),
                pltpu.VMEM((8, m), jnp.float32),
                pltpu.VMEM((m // S, m, S), jnp.float32),
                pltpu.VMEM((3, B, B), jnp.float32),
                pltpu.VMEM((2 * B, B), jnp.float32),
                pltpu.VMEM((4, m, S), jnp.bfloat16),
                pltpu.VMEM((2, m, m), jnp.bfloat16),
                pltpu.VMEM((2, S, S), jnp.bfloat16),
                pltpu.VMEM((4, count, S), jnp.bfloat16),
                pltpu.VMEM((count, B), jnp.float32),
            ],
        ),
        out_shape=(pltpu.VMEM((m // S, count, S), jnp.float32), jax.ShapeDtypeStruct((2, m), jnp.float32)),
        compiler_params=pltpu.CompilerParams(vmem_limit_bytes=40 << 20),
        name="nystrom",
    )(info, low[0], *pieces, kept, ridge[None, :])

    total = count
    for bit in bits:
        other = exchange(stat, bit)
        delta = other[0] - stat[0]
        stat = jnp.stack([0.5 * (stat[0] + other[0]), stat[1] + other[1] + jnp.square(delta) * (0.5 * total)])
        total *= 2
    gain = 1.0 / jnp.sqrt(stat[1:2] / total + 1e-05)
    steps = 8
    return pl.pallas_call(
        standardize,
        in_specs=[vmem] * 3,
        out_specs=pl.BlockSpec(memory_space=pl.ANY),
        scratch_shapes=[pltpu.VMEM((steps, count // steps, m), jnp.bfloat16), pltpu.SemaphoreType.DMA((steps,))],
        out_shape=jax.ShapeDtypeStruct((count, m), jnp.bfloat16),
        compiler_params=pltpu.CompilerParams(vmem_limit_bytes=16 << 20),
        name="standardize",
    )(raw, stat[0:1], gain)


def solution(mesh):
    placed = (P(AXES, None), P(), P())
    return jax.shard_map(shards, mesh=mesh, in_specs=placed, out_specs=P(AXES, None), check_vma=False)
```
